32 devices in a mesh: row: 2 (over y), col: 16 (over z, x, core).
Axes of the slice: x: 2, y: 2, z: 4, core: 2. Of those that a mesh axis runs over, the one named last changes fastest.
Arguments:
- queries: bfloat16 [512, 4096], P(('row', 'col')), may hold values from -1.25 to 1.25
- passages: bfloat16 [8192, 4096], P(('col', 'row')), may hold values from -0.375 to 0.375
- positives: int32 [512], P('row'), may hold values from 0 to 8191, as said below
- hard_negatives: int32 [512, 7], P('row'), may hold values from 0 to 8191, as said below
- thresholds: float32 [512], P('row'), may hold values from 0.1 to 2
Outputs:
- row_losses: float32 [512], P(('row', 'col'))
- grad_queries: float32 [512, 4096], P(('row', 'col'))
- grad_passages: float32 [8192, 4096], P(('col', 'row'))
The draws below stay inside these ranges and needn't reach their ends.
Inputs may be any that keep to these rules, and one draw needn't show every extreme that they name: `positives`: each query's positive passage. `hard_negatives`: passages mined for each query; ids may repeat or equal the query's positive.
All inputs are finite; a program needn't handle non-finite values.
Results may differ from the reference program's by a relative error of at most 0.0023.
Values may be sent and summed in bfloat16 or wider, within the bound.
A program may use at most 64 MiB of HBM per device.

```python
import math
import jax
import jax.numpy as jnp
from jax import lax

D = 4096
NEGS = 7
NQ = 512
NP = 8192


def integer_tables(key):
    positives = jax.random.randint(jax.random.fold_in(key, 11), (NQ,), 0, NP)
    mined_ids = jax.random.randint(jax.random.fold_in(key, 12), (NQ, NEGS), 0, NP)
    return (positives, mined_ids)


def log_even(key, shape, lower, upper):
    return jnp.exp(jax.random.uniform(key, shape, jnp.float32, math.log(lower), math.log(upper)))


def embedding_tables(key):
    positives, mined_ids = integer_tables(key)
    unit_scale = D ** (-0.5)
    passage_noise = jax.random.truncated_normal(jax.random.fold_in(key, 21), -6.0, 6.0, (NP, D), jnp.float32) * unit_scale
    scales = log_even(jax.random.fold_in(key, 22), (NP, 1), 0.7, 1.4)
    passages = passage_noise * scales
    query_noise = jax.random.truncated_normal(jax.random.fold_in(key, 24), -6.0, 6.0, (NQ, D), jnp.float32) * unit_scale
    linked = 0.06 * passages[positives] + 0.05 * jnp.sum(passages[mined_ids], axis=1)
    query_scale = log_even(jax.random.fold_in(key, 25), (NQ, 1), 0.6, 1.6)
    queries = (query_noise + linked) * query_scale
    queries = jnp.clip(queries, -80.0 * unit_scale, 80.0 * unit_scale)
    passages = jnp.clip(passages, -24.0 * unit_scale, 24.0 * unit_scale)
    return (queries, passages)


def draw_queries(key, part):
    return embedding_tables(key)[0].astype(jnp.bfloat16)


def draw_passages(key, part):
    return embedding_tables(key)[1].astype(jnp.bfloat16)


def draw_positives(key, part):
    return integer_tables(key)[0]


def draw_hard_negatives(key, part):
    return integer_tables(key)[1]


def level_of(stream_key, extent, cuts, low, largest):
    loudness, own = 1.0, jax.random.fold_in(stream_key, 6)
    for axis_at, blocks in cuts:
        draws = jnp.exp(jax.random.uniform(jax.random.fold_in(own, axis_at), (blocks,), jnp.float32, low / len(cuts), largest / len(cuts)))
        loudness = loudness * jnp.repeat(draws, extent[axis_at] // blocks).reshape([-1 if axis == axis_at else 1 for axis in range(len(extent))])
    return loudness


def setup_inputs(seed: int = 0) -> dict:
    keys = jax.random.split(jax.random.key(seed), 6)
    return {
        "queries": draw_queries(jax.random.fold_in(keys[5], 71), 0),
        "passages": draw_passages(jax.random.fold_in(keys[5], 71), 0),
        "positives": draw_positives(jax.random.fold_in(keys[5], 71), 0),
        "hard_negatives": draw_hard_negatives(jax.random.fold_in(keys[5], 71), 0),
        "thresholds": jnp.clip(jnp.exp(math.log(2.0) - 2.9957323 * jax.random.uniform(keys[4], (NQ,), jnp.float32) ** level_of(keys[4], (NQ,), ((0, 2),), -0.2, 0.2)), 0.1, 2.0),
    }


inv_temp = 50.0
sharpness = 4.0


def reference(queries, passages, positives, hard_negatives, thresholds):
    scores = jnp.dot(queries, passages.T, preferred_element_type=jnp.float32) * inv_temp
    columns = lax.iota(jnp.int32, passages.shape[0])
    positive_mask = positives[:, None] == columns[None, :]
    kept_mask = positive_mask
    for mined_slot in range(NEGS):
        kept_mask = kept_mask | (hard_negatives[:, mined_slot:mined_slot + 1] == columns[None, :])
    picked = jnp.sum(jnp.where(positive_mask, scores, 0.0), axis=1)
    penalty = jax.nn.softplus(sharpness * (scores - picked[:, None] - thresholds[:, None]))
    logits = jnp.where(kept_mask, scores, scores - penalty)
    row_top = jnp.max(logits, axis=1)
    shifted = jnp.exp(logits - row_top[:, None])
    denominator = jnp.sum(shifted, axis=1)
    row_losses = row_top + jnp.log(denominator) - picked
    grad_scores = ((shifted / denominator[:, None] - positive_mask.astype(jnp.float32)) * inv_temp).astype(jnp.bfloat16)
    grad_queries = jnp.dot(grad_scores, passages, preferred_element_type=jnp.float32)
    grad_passages = jnp.dot(grad_scores.T, queries, preferred_element_type=jnp.float32)
    return row_losses, grad_queries, grad_passages
```

```python
import functools
import jax
import jax.numpy as jnp
from jax import lax
from jax.experimental import pallas as pl
from jax.experimental.pallas import tpu as pltpu
from jax.sharding import PartitionSpec as P

inv_temp = 50.0
sharpness = 4.0


def combined_all(part, axis, combine):
    gathered = jax.tree.map(lambda a: lax.all_gather(a, axis), part)

    def take(source):
        return jax.tree.map(lambda a: lax.dynamic_index_in_dim(a, source, 0, False), gathered)

    return lax.fori_loop(
        1, lax.axis_size(axis), lambda source, state: combine(state, take(source)), take(0)
    )


def pair_merge(left_pair, right_pair):
    left_top, left_total = left_pair
    right_top, right_total = right_pair
    joined = jnp.maximum(left_top, right_top)
    return (
        joined,
        left_total * jnp.exp(left_top - joined) + right_total * jnp.exp(right_top - joined),
    )


def general_plan(queries, passages, positives, hard_negatives, thresholds):
    query_block = lax.all_gather(queries, "col", axis=0, tiled=True)
    passage_block = lax.all_gather(passages, "row", axis=0, tiled=True)
    block_width = passage_block.shape[0]
    query_rows = queries.shape[0]
    scores = jnp.dot(query_block, passage_block.T, preferred_element_type=jnp.float32) * inv_temp
    columns = lax.axis_index("col") * block_width + lax.iota(jnp.int32, block_width)
    positive_mask = positives[:, None] == columns[None, :]
    kept_mask = positive_mask
    for mined_slot in range(hard_negatives.shape[1]):
        kept_mask = kept_mask | (hard_negatives[:, mined_slot : mined_slot + 1] == columns[None, :])
    picked = lax.psum(jnp.sum(jnp.where(positive_mask, scores, 0.0), axis=1), "col")
    penalty = jax.nn.softplus(sharpness * (scores - picked[:, None] - thresholds[:, None]))
    logits = jnp.where(kept_mask, scores, scores - penalty)
    local_top = jnp.max(logits, axis=1)
    local_exp = jnp.exp(logits - local_top[:, None])
    row_top, denominator = combined_all((local_top, jnp.sum(local_exp, axis=1)), "col", pair_merge)
    shifted = local_exp * jnp.exp(local_top - row_top)[:, None]
    losses = row_top + jnp.log(denominator) - picked
    row_losses = lax.dynamic_slice_in_dim(losses, lax.axis_index("col") * query_rows, query_rows, 0)
    grad_scores = (
        (shifted / denominator[:, None] - positive_mask.astype(jnp.float32)) * inv_temp
    ).astype(jnp.bfloat16)
    query_full = jnp.dot(grad_scores, passage_block, preferred_element_type=jnp.float32)
    grad_queries = lax.psum_scatter(query_full, "col", scatter_dimension=0, tiled=True)
    passage_full = lax.dot_general(
        grad_scores, query_block, (((0,), (0,)), ((), ())), preferred_element_type=jnp.float32
    )
    grad_passages = lax.psum_scatter(passage_full, "row", scatter_dimension=0, tiled=True)
    return (row_losses, grad_queries, grad_passages)


cores = 2
lane = 128
fields = 16
MESH = pl.DeviceIdType.MESH


def step_kernel(
    rows, wide, deep, negs,
    q_ref, p_ref, positives_ref, mined_ref, thresholds_ref,
    loss_ref, gq_ref, gp_ref,
    p_own, positives_own, mined_own, thresholds_own,
    q_all, p_mate, mined_wide, meta_ref, meta_all, scores, pick_out, pick_all, stat_out, stat_all,
    part, part_low, gp_out, gp_in,
    diag_in_y, diag_in_x, merge_x, merge_y, in_x, in_y, plane, z_out, z_in, z_out_full, z_in_full,
    load_sem, own_send, fwd_send, diag_send, q_recv,
    mate_send, mate_recv, meta_send, meta_recv,
    pick_send, pick_recv, stat_send, stat_recv,
    rd_send, rd_recv, ru_send, ru_recv, rm_send, rm_recv, z_send, z_recv,
):
    y = lax.axis_index("row")
    col = lax.axis_index("col")
    core = lax.rem(col, cores)
    chip = col // cores
    z = chip // wide
    x = lax.rem(chip, wide)
    block, depth = q_ref.shape
    half = depth // 2
    own = p_ref.shape[0]
    groups = rows * deep * wide
    queries = groups * block

    def device(yy, zz, xx, cc=None):
        return (yy, (zz * wide + xx) * cores + (core if cc is None else cc))

    def slot(yy, zz, xx):
        return (yy * deep + zz) * wide + xx

    def span(g):
        return pl.ds(pl.multiple_of(g * block, block), block)

    def turn(at, by, size):
        return lax.rem(at + by, size)

    def send(src, dst, send_sem, recv_sem, to):
        copy = pltpu.make_async_remote_copy(
            src_ref=src, dst_ref=dst, send_sem=send_sem, recv_sem=recv_sem,
            device_id=to, device_id_type=MESH,
        )
        copy.start()
        sent.append(copy)

    def landed(ref, sem):
        pltpu.make_async_copy(ref, ref, sem).wait()

    sent = []
    waits = []
    left, right = pl.ds(0, half), pl.ds(half, half)
    yn, xn = turn(y, 1, rows), turn(x, 1, wide)
    me = slot(y, z, x)
    mate = device(y, z, x, 1 - core)
    across, along = device(y, z, xn), device(yn, z, x)
    peers = [
        (turn(y, a, rows), turn(z, b, deep), turn(x, d, wide))
        for b in range(deep) for a in range(rows) for d in range(wide) if a + b + d
    ]
    steps = 4
    width = depth // steps

    def columns(k):
        return pl.ds(k * width, width)

    q_load = pltpu.make_async_copy(q_ref, q_all.at[span(me)], load_sem.at[0])
    p_load = pltpu.make_async_copy(p_ref, p_own, load_sem.at[1])
    tables = [
        pltpu.make_async_copy(positives_ref, positives_own, load_sem.at[2]),
        pltpu.make_async_copy(mined_ref, mined_own, load_sem.at[3]),
        pltpu.make_async_copy(thresholds_ref, thresholds_own, load_sem.at[4]),
    ]
    q_load.start()
    p_load.start()
    for table in tables:
        table.start()

    has_up, has_down = z < deep - 1, z > 0
    above = device(y, jnp.minimum(z + 1, deep - 1), x)
    below = device(y, jnp.maximum(z - 1, 0), x)
    barrier = pltpu.get_barrier_semaphore()
    for to in (across, along, mate):
        pl.semaphore_signal(barrier, inc=1, device_id=to, device_id_type=MESH)

    @pl.when(has_up)
    def _():
        pl.semaphore_signal(barrier, inc=1, device_id=above, device_id_type=MESH)

    @pl.when(has_down)
    def _():
        pl.semaphore_signal(barrier, inc=1, device_id=below, device_id_type=MESH)

    pl.semaphore_wait(barrier, 3 + jnp.where(has_up, 1, 0) + jnp.where(has_down, 1, 0))
    q_load.wait()

    def pass_on(g, k, sem, to):
        ref = q_all.at[span(g), columns(k)]
        pltpu.make_async_remote_copy(
            src_ref=ref, dst_ref=ref, send_sem=sem, recv_sem=q_recv.at[g, k],
            device_id=to, device_id_type=MESH,
        ).start()

    whole = q_all.at[span(me)]
    for k in range(steps):
        @pl.when(has_up)
        def _():
            pass_on(me, k, own_send.at[0], above)

        @pl.when(has_down)
        def _():
            pass_on(me, k, own_send.at[1], below)

        pass_on(me, k, own_send.at[2], across)
        pass_on(me, k, own_send.at[3], along)
    waits.append((has_up, whole, own_send.at[0]))
    waits.append((has_down, whole, own_send.at[1]))
    waits.append((None, whole, own_send.at[2]))
    waits.append((None, whole, own_send.at[3]))
    p_load.wait()
    send(p_own, p_mate, mate_send.at[0], mate_recv.at[0], mate)
    for table in tables:
        table.wait()

    def mine(table):
        return jnp.concatenate(
            [table[(m * cores) * block : (m * cores + 1) * block] for m in range(deep * wide)], axis=0
        ), jnp.concatenate(
            [table[(m * cores + 1) * block : (m * cores + 2) * block] for m in range(deep * wide)], axis=0
        )

    mined_wide[...] = jnp.zeros_like(mined_wide)
    mined_wide[:negs, :] = mined_own[...].astype(jnp.float32)
    mined_wide[fields // 2 : fields // 2 + 1, :] = positives_own[...].astype(jnp.float32)
    mined_wide[fields // 2 + 1 : fields // 2 + 2, :] = thresholds_own[...]
    one_first, one_second = mine(jnp.transpose(mined_wide[...]))
    meta_ref[...] = jnp.transpose(jnp.where(core == 0, one_first, one_second))[:fields]
    meta_all[y] = meta_ref[...]
    send(meta_ref, meta_all.at[y], meta_send, meta_recv, device(yn, z, x))

    def column_step(h, up):
        source = z - h if up else z + h
        inside = source >= 0 if up else source < deep
        more = has_up if up else has_down
        far = above if up else below
        g = slot(y, jnp.clip(source, 0, deep - 1), x)
        sems = fwd_send.at[0 if up else 1, h - 1]

        def arrive(k):
            @pl.when(inside)
            def _():
                landed(q_all.at[span(g), columns(k)], q_recv.at[g, k])

                @pl.when(more)
                def _():
                    pass_on(g, k, sems.at[0], far)

                pass_on(g, k, sems.at[1], across)
                pass_on(g, k, sems.at[2], along)

        waits.append((inside & more, whole, sems.at[0]))
        waits.append((inside, whole, sems.at[1]))
        waits.append((inside, whole, sems.at[2]))
        return arrive

    def corner_step(source, inside, sem):
        at = jnp.clip(source, 0, deep - 1)
        gx, gy = slot(y, at, xn), slot(yn, at, x)

        def forward(k):
            g, to, n = (gx, along, 0) if k % 2 == 0 else (gy, across, 1)

            def go():
                landed(q_all.at[span(g), columns(k)], q_recv.at[g, k])
                pass_on(g, k, sem.at[n], to)

            if inside is None:
                go()
            else:
                pl.when(inside)(go)

        waits.append((inside, q_all.at[span(me), left], sem.at[0]))
        waits.append((inside, q_all.at[span(me), left], sem.at[1]))
        return forward

    corners = [corner_step(z, None, diag_send.at[0, 0])]
    for h in range(1, deep):
        arrivals = [column_step(h, True), column_step(h, False)]
        for k in range(steps):
            for go in arrivals:
                go(k)
            for go in corners:
                go(k)
        corners = [
            corner_step(z - h, z - h >= 0, diag_send.at[0, h]),
            corner_step(z + h, z + h < deep, diag_send.at[1, h]),
        ]
    for k in range(steps):
        for go in corners:
            go(k)
    landed(p_mate, mate_recv.at[0])
    landed(meta_all.at[yn], meta_recv)

    for k in range(steps):
        for b in range(deep):
            zb = turn(z, b, deep)
            g = slot(yn, zb, x) if k % 2 == 0 else slot(y, zb, xn)
            gd = slot(yn, zb, xn)
            landed(q_all.at[span(g), columns(k)], q_recv.at[g, k])
            landed(q_all.at[span(gd), columns(k)], q_recv.at[gd, k])
        ks = columns(k)
        q_piece = q_all[:, ks]
        for at, p_part in ((0, p_own), (own, p_mate)):
            value = lax.dot_general(
                p_part[:, ks], q_piece, (((1,), (1,)), ((), ())), preferred_element_type=jnp.float32
            )
            if k:
                scores[at : at + own, :] += value
            else:
                scores[at : at + own, :] = value

    mt = jnp.concatenate([meta_all[a] for a in range(rows)], axis=1)
    at = lax.broadcasted_iota(jnp.int32, (2 * own, queries), 0)
    first = ((chip * cores + core) * rows + y) * own
    second = ((chip * cores + (1 - core)) * rows + y) * own
    ids = jnp.where(at < own, at + first, at - own + second).astype(jnp.float32)
    sc = scores[...] * inv_temp
    positive = ids == mt[fields // 2 : fields // 2 + 1, :]
    picked_here = jnp.sum(jnp.where(positive, sc, 0.0), axis=0, keepdims=True)
    pick_out[...] = picked_here
    for n, peer in enumerate(peers):
        send(pick_out, pick_all.at[me], pick_send.at[n], pick_recv.at[me], device(*peer))
    kept = positive
    for n in range(negs):
        kept = kept | (ids == mt[n : n + 1, :])
    pick_all[me] = picked_here
    for peer in peers:
        g = slot(*peer)
        landed(pick_all.at[g], pick_recv.at[g])
    picked = jnp.sum(pick_all[...], axis=0)
    v = sharpness * (sc - picked - mt[fields // 2 + 1 : fields // 2 + 2, :])
    penalty = jnp.maximum(v, 0.0) + jnp.log1p(jnp.exp(-jnp.abs(v)))
    logits = jnp.where(kept, sc, sc - penalty)
    top_here = jnp.max(logits, axis=0, keepdims=True)
    grown = jnp.exp(logits - top_here)
    sum_here = jnp.sum(grown, axis=0, keepdims=True)
    stat_out[...] = jnp.concatenate([top_here, sum_here], axis=1)
    for n, peer in enumerate(peers):
        send(stat_out, stat_all.at[me], stat_send.at[n], stat_recv.at[me], device(*peer))
    stat_all[me] = stat_out[...]
    for peer in peers:
        g = slot(*peer)
        landed(stat_all.at[g], stat_recv.at[g])
    stats = stat_all[...]
    tops, sums = stats[:, :, :queries], stats[:, :, queries:]
    row_top = jnp.max(tops, axis=0)
    total = jnp.sum(sums * jnp.exp(tops - row_top[None]), axis=0)
    losses = jnp.broadcast_to(row_top + jnp.log(total) - picked, (8, queries))
    loss_ref[...] = pltpu.roll(losses, lax.rem(queries - me * block, queries), 1)[:1, :lane]
    factor = jnp.exp(top_here - row_top) / total
    grad = ((grown * factor - positive.astype(jnp.float32)) * inv_temp).astype(jnp.bfloat16)
    grad_t = jnp.transpose(grad)

    cuts = 8
    cut = depth // cuts

    @pl.loop(0, cuts)
    def _(k):
        ks = pl.ds(pl.multiple_of(k * cut, lane), cut)
        value = jnp.dot(grad_t[:, :own], p_own[:, ks], preferred_element_type=jnp.float32) + jnp.dot(
            grad_t[:, own:], p_mate[:, ks], preferred_element_type=jnp.float32
        )
        part[:, ks] = value
        part_low[:, ks] = value.astype(jnp.bfloat16)

    order = list(range(1, deep)) + [0]

    def diagonal(b):
        gd = slot(yn, turn(z, b, deep), xn)
        send(part_low.at[span(gd), left], diag_in_y.at[b], rd_send.at[b, 0], rd_recv.at[b, 0], device(yn, z, x))
        send(part_low.at[span(gd), right], diag_in_x.at[b], rd_send.at[b, 1], rd_recv.at[b, 1], device(y, z, xn))

    def plain(b):
        zb = turn(z, b, deep)
        gx, gy = slot(y, zb, xn), slot(yn, zb, x)
        send(part_low.at[span(gx), right], in_x.at[b, :, right], ru_send.at[b, 0], ru_recv.at[b, 0], device(y, z, xn))
        send(part_low.at[span(gy), left], in_y.at[b, :, left], ru_send.at[b, 1], ru_recv.at[b, 1], device(yn, z, x))

    def merged(b):
        zb = turn(z, b, deep)
        gx, gy = slot(y, zb, xn), slot(yn, zb, x)
        landed(diag_in_y.at[b], rd_recv.at[b, 0])
        merge_x[b] = (part[span(gx), left] + diag_in_y[b].astype(jnp.float32)).astype(jnp.bfloat16)
        send(merge_x.at[b], in_x.at[b, :, left], rm_send.at[b, 0], rm_recv.at[b, 0], device(y, z, xn))
        landed(diag_in_x.at[b], rd_recv.at[b, 1])
        merge_y[b] = (part[span(gy), right] + diag_in_x[b].astype(jnp.float32)).astype(jnp.bfloat16)
        send(merge_y.at[b], in_y.at[b, :, right], rm_send.at[b, 1], rm_recv.at[b, 1], device(yn, z, x))

    def z_buffers(b):
        return (z_out_full, z_in_full) if b in (1, deep - 1) else (z_out, z_in)

    def settle(b):
        zb = turn(z, b, deep)
        landed(in_x.at[b, :, right], ru_recv.at[b, 0])
        landed(in_y.at[b, :, left], ru_recv.at[b, 1])
        landed(in_x.at[b, :, left], rm_recv.at[b, 0])
        landed(in_y.at[b, :, right], rm_recv.at[b, 1])
        value = part[span(slot(y, zb, x)), :] + in_x[b].astype(jnp.float32) + in_y[b].astype(jnp.float32)
        if b:
            out, into = z_buffers(b)
            out[b] = value.astype(out.dtype)
            send(out.at[b], into.at[b], z_send.at[b], z_recv.at[b], device(y, zb, x))
        else:
            plane[...] = value

    diagonal(order[0])
    diagonal(order[1])
    plain(order[0])

    @pl.loop(0, cuts)
    def _(k):
        ks = pl.ds(pl.multiple_of(k * cut, lane), cut)
        gp_out[:, ks] = jnp.dot(grad[own:, :], q_all[:, ks], preferred_element_type=jnp.float32)

    send(gp_out, gp_in, mate_send.at[1], mate_recv.at[1], mate)

    for n, b in enumerate(order):
        merged(b)
        if n + 2 < deep:
            diagonal(order[n + 2])
        if n + 1 < deep:
            plain(order[n + 1])
        if n:
            settle(order[n - 1])

    @pl.loop(0, cuts)
    def _(k):
        ks = pl.ds(pl.multiple_of(k * cut, lane), cut)
        gp_ref[:, ks] = jnp.dot(grad[:own, :], q_all[:, ks], preferred_element_type=jnp.float32)

    landed(gp_in, mate_recv.at[1])

    @pl.loop(0, cuts)
    def _(k):
        ks = pl.ds(pl.multiple_of(k * cut, lane), cut)
        gp_ref[:, ks] += gp_in[:, ks]

    settle(0)
    value = plane[...]
    for b in range(1, deep):
        into = z_buffers(b)[1]
        landed(into.at[b], z_recv.at[b])
        value = value + into[b].astype(jnp.float32)
    gq_ref[...] = value
    for inside, ref, sem in waits:
        if inside is None:
            landed(ref, sem)
        else:
            pl.when(inside)(functools.partial(landed, ref, sem))
    for copy in sent:
        copy.wait_send()


def on_device(queries, passages, positives, hard_negatives, thresholds):
    rows, columns = lax.axis_size("row"), lax.axis_size("col")
    wide = rows
    deep = columns // (cores * wide)
    block, depth = queries.shape
    own = passages.shape[0]
    negs = hard_negatives.shape[1]
    run = deep * wide * block
    fits = rows == 2 and columns % (cores * wide) == 0 and deep > 1
    fits = fits and block % 16 == 0 and run % lane == 0 and negs <= fields // 2 and depth % 1024 == 0
    if not fits:
        return general_plan(queries, passages, positives, hard_negatives, thresholds)
    groups = rows * deep * wide
    total = groups * block
    half = depth // 2
    low, full = jnp.bfloat16, jnp.float32
    dma = pltpu.SemaphoreType.DMA
    losses, grad_queries, grad_passages = pl.pallas_call(
        functools.partial(step_kernel, rows, wide, deep, negs),
        out_shape=(
            jax.ShapeDtypeStruct((1, lane), full),
            jax.ShapeDtypeStruct((block, depth), full),
            jax.ShapeDtypeStruct((own, depth), full),
        ),
        in_specs=[pl.BlockSpec(memory_space=pltpu.HBM)] * 5,
        out_specs=[pl.BlockSpec(memory_space=pltpu.VMEM)] * 3,
        scratch_shapes=[
            pltpu.VMEM((own, depth), low),
            pltpu.VMEM((1, positives.shape[0]), jnp.int32),
            pltpu.VMEM((negs, positives.shape[0]), jnp.int32),
            pltpu.VMEM((1, positives.shape[0]), full),
            pltpu.VMEM((total, depth), low),
            pltpu.VMEM((own, depth), low),
            pltpu.VMEM((lane, columns * block), full),
            pltpu.VMEM((fields, run), full),
            pltpu.VMEM((rows, fields, run), full),
            pltpu.VMEM((cores * own, total), full),
            pltpu.VMEM((1, total), full),
            pltpu.VMEM((groups, 1, total), full),
            pltpu.VMEM((1, 2 * total), full),
            pltpu.VMEM((groups, 1, 2 * total), full),
            pltpu.VMEM((total, depth), full),
            pltpu.VMEM((total, depth), low),
            pltpu.VMEM((own, depth), full),
            pltpu.VMEM((own, depth), full),
            pltpu.VMEM((deep, block, half), low),
            pltpu.VMEM((deep, block, half), low),
            pltpu.VMEM((deep, block, half), low),
            pltpu.VMEM((deep, block, half), low),
            pltpu.VMEM((deep, block, depth), low),
            pltpu.VMEM((deep, block, depth), low),
            pltpu.VMEM((block, depth), full),
            pltpu.VMEM((deep, block, depth), low),
            pltpu.VMEM((deep, block, depth), low),
            pltpu.VMEM((deep, block, depth), full),
            pltpu.VMEM((deep, block, depth), full),
            dma((5,)), dma((4,)), dma((2, deep, 3)), dma((2, deep, 2)), dma((groups, 4)),
            dma((2,)), dma((2,)), dma, dma,
            dma((groups,)), dma((groups,)), dma((groups,)), dma((groups,)),
            dma((deep, 2)), dma((deep, 2)), dma((deep, 2)), dma((deep, 2)),
            dma((deep, 2)), dma((deep, 2)), dma((deep,)), dma((deep,)),
        ],
        compiler_params=pltpu.CompilerParams(
            collective_id=0, has_side_effects=True, vmem_limit_bytes=44 * 1024 * 1024
        ),
    )(queries, passages, positives[None], hard_negatives.T, thresholds[None])
    return (losses[0, :block], grad_queries, grad_passages)


def solution(mesh):
    placed = (P(("row", "col"), None), P(("col", "row"), None), P("row"), P("row", None), P("row"))
    return jax.shard_map(
        on_device,
        mesh=mesh,
        in_specs=placed,
        out_specs=(P(("row", "col")), P(("row", "col"), None), P(("col", "row"), None)),
        check_vma=False,
    )
```

```python
import functools
import jax
import jax.numpy as jnp
from jax import lax
from jax.experimental import pallas as pl
from jax.experimental.pallas import tpu as pltpu
from jax.sharding import PartitionSpec as P

inv_temp = 50.0
sharpness = 4.0


def combined_all(part, axis, combine):
    gathered = jax.tree.map(lambda a: lax.all_gather(a, axis), part)

    def take(source):
        return jax.tree.map(lambda a: lax.dynamic_index_in_dim(a, source, 0, False), gathered)

    return lax.fori_loop(
        1, lax.axis_size(axis), lambda source, state: combine(state, take(source)), take(0)
    )


def pair_merge(left_pair, right_pair):
    left_top, left_total = left_pair
    right_top, right_total = right_pair
    joined = jnp.maximum(left_top, right_top)
    return (
        joined,
        left_total * jnp.exp(left_top - joined) + right_total * jnp.exp(right_top - joined),
    )


def general_plan(queries, passages, positives, hard_negatives, thresholds):
    query_block = lax.all_gather(queries, "col", axis=0, tiled=True)
    passage_block = lax.all_gather(passages, "row", axis=0, tiled=True)
    block_width = passage_block.shape[0]
    query_rows = queries.shape[0]
    scores = jnp.dot(query_block, passage_block.T, preferred_element_type=jnp.float32) * inv_temp
    columns = lax.axis_index("col") * block_width + lax.iota(jnp.int32, block_width)
    positive_mask = positives[:, None] == columns[None, :]
    kept_mask = positive_mask
    for mined_slot in range(hard_negatives.shape[1]):
        kept_mask = kept_mask | (hard_negatives[:, mined_slot : mined_slot + 1] == columns[None, :])
    picked = lax.psum(jnp.sum(jnp.where(positive_mask, scores, 0.0), axis=1), "col")
    penalty = jax.nn.softplus(sharpness * (scores - picked[:, None] - thresholds[:, None]))
    logits = jnp.where(kept_mask, scores, scores - penalty)
    local_top = jnp.max(logits, axis=1)
    local_exp = jnp.exp(logits - local_top[:, None])
    row_top, denominator = combined_all((local_top, jnp.sum(local_exp, axis=1)), "col", pair_merge)
    shifted = local_exp * jnp.exp(local_top - row_top)[:, None]
    losses = row_top + jnp.log(denominator) - picked
    row_losses = lax.dynamic_slice_in_dim(losses, lax.axis_index("col") * query_rows, query_rows, 0)
    grad_scores = (
        (shifted / denominator[:, None] - positive_mask.astype(jnp.float32)) * inv_temp
    ).astype(jnp.bfloat16)
    query_full = jnp.dot(grad_scores, passage_block, preferred_element_type=jnp.float32)
    grad_queries = lax.psum_scatter(query_full, "col", scatter_dimension=0, tiled=True)
    passage_full = lax.dot_general(
        grad_scores, query_block, (((0,), (0,)), ((), ())), preferred_element_type=jnp.float32
    )
    grad_passages = lax.psum_scatter(passage_full, "row", scatter_dimension=0, tiled=True)
    return (row_losses, grad_queries, grad_passages)


cores = 2
lane = 128
fields = 16
MESH = pl.DeviceIdType.MESH


def step_kernel(
    rows, wide, deep, negs,
    q_ref, p_ref, positives_ref, mined_ref, thresholds_ref,
    loss_ref, gq_ref, gp_ref,
    p_own, positives_own, mined_own, thresholds_own,
    q_all, p_mate, mined_wide, meta_ref, meta_all, scores, pick_out, pick_all, stat_out, stat_all,
    part, part_low, gp_out, gp_in,
    diag_in_y, diag_in_x, merge_x, merge_y, in_x, in_y, plane, z_out, z_in, z_out_full, z_in_full,
    load_sem, own_send, fwd_send, diag_send, q_recv,
    mate_send, mate_recv, meta_send, meta_recv,
    pick_send, pick_recv, stat_send, stat_recv,
    rd_send, rd_recv, ru_send, ru_recv, rm_send, rm_recv, z_send, z_recv, turn_sem,
):
    y = lax.axis_index("row")
    col = lax.axis_index("col")
    core = lax.rem(col, cores)
    chip = col // cores
    z = chip // wide
    x = lax.rem(chip, wide)
    block, depth = q_ref.shape
    half = depth // 2
    own = p_ref.shape[0]
    groups = rows * deep * wide
    queries = groups * block

    def device(yy, zz, xx, cc=None):
        return (yy, (zz * wide + xx) * cores + (core if cc is None else cc))

    def slot(yy, zz, xx):
        return (yy * deep + zz) * wide + xx

    def span(g):
        return pl.ds(pl.multiple_of(g * block, block), block)

    def turn(at, by, size):
        return lax.rem(at + by, size)

    def send(src, dst, send_sem, recv_sem, to):
        copy = pltpu.make_async_remote_copy(
            src_ref=src, dst_ref=dst, send_sem=send_sem, recv_sem=recv_sem,
            device_id=to, device_id_type=MESH,
        )
        copy.start()
        sent.append(copy)

    def landed(ref, sem):
        pltpu.make_async_copy(ref, ref, sem).wait()

    sent = []
    waits = []
    left, right = pl.ds(0, half), pl.ds(half, half)
    yn, xn = turn(y, 1, rows), turn(x, 1, wide)
    me = slot(y, z, x)
    mate = device(y, z, x, 1 - core)
    across, along = device(y, z, xn), device(yn, z, x)
    peers = [
        (turn(y, a, rows), turn(z, b, deep), turn(x, d, wide))
        for b in range(deep) for a in range(rows) for d in range(wide) if a + b + d
    ]
    steps = 4
    width = depth // steps

    def columns(k):
        return pl.ds(k * width, width)

    q_load = pltpu.make_async_copy(q_ref, q_all.at[span(me)], load_sem.at[0])
    p_load = pltpu.make_async_copy(p_ref, p_own, load_sem.at[1])
    tables = [
        pltpu.make_async_copy(positives_ref, positives_own, load_sem.at[2]),
        pltpu.make_async_copy(mined_ref, mined_own, load_sem.at[3]),
        pltpu.make_async_copy(thresholds_ref, thresholds_own, load_sem.at[4]),
    ]
    q_load.start()
    p_load.start()
    for table in tables:
        table.start()

    has_up, has_down = z < deep - 1, z > 0
    above = device(y, jnp.minimum(z + 1, deep - 1), x)
    below = device(y, jnp.maximum(z - 1, 0), x)
    barrier = pltpu.get_barrier_semaphore()
    for to in (across, along, mate):
        pl.semaphore_signal(barrier, inc=1, device_id=to, device_id_type=MESH)

    @pl.when(has_up)
    def _():
        pl.semaphore_signal(barrier, inc=1, device_id=above, device_id_type=MESH)

    @pl.when(has_down)
    def _():
        pl.semaphore_signal(barrier, inc=1, device_id=below, device_id_type=MESH)

    pl.semaphore_wait(barrier, 3 + jnp.where(has_up, 1, 0) + jnp.where(has_down, 1, 0))
    q_load.wait()

    def pass_on(g, k, sem, to):
        ref = q_all.at[span(g), columns(k)]
        pltpu.make_async_remote_copy(
            src_ref=ref, dst_ref=ref, send_sem=sem, recv_sem=q_recv.at[g, k],
            device_id=to, device_id_type=MESH,
        ).start()

    whole = q_all.at[span(me)]

    @pl.when(core == 0)
    def _():
        pl.semaphore_wait(turn_sem, 1)

    for k in range(steps):
        @pl.when(has_up)
        def _():
            pass_on(me, k, own_send.at[0], above)

        @pl.when(has_down)
        def _():
            pass_on(me, k, own_send.at[1], below)

        pass_on(me, k, own_send.at[2], across)
        pass_on(me, k, own_send.at[3], along)
    waits.append((has_up, whole, own_send.at[0]))
    waits.append((has_down, whole, own_send.at[1]))
    waits.append((None, whole, own_send.at[2]))
    waits.append((None, whole, own_send.at[3]))
    p_load.wait()
    send(p_own, p_mate, mate_send.at[0], mate_recv.at[0], mate)
    for table in tables:
        table.wait()

    def mine(table):
        return jnp.concatenate(
            [table[(m * cores) * block : (m * cores + 1) * block] for m in range(deep * wide)], axis=0
        ), jnp.concatenate(
            [table[(m * cores + 1) * block : (m * cores + 2) * block] for m in range(deep * wide)], axis=0
        )

    mined_wide[...] = jnp.zeros_like(mined_wide)
    mined_wide[:negs, :] = mined_own[...].astype(jnp.float32)
    mined_wide[fields // 2 : fields // 2 + 1, :] = positives_own[...].astype(jnp.float32)
    mined_wide[fields // 2 + 1 : fields // 2 + 2, :] = thresholds_own[...]
    one_first, one_second = mine(jnp.transpose(mined_wide[...]))
    meta_ref[...] = jnp.transpose(jnp.where(core == 0, one_first, one_second))[:fields]
    meta_all[y] = meta_ref[...]
    send(meta_ref, meta_all.at[y], meta_send, meta_recv, device(yn, z, x))

    def column_step(h, up):
        source = z - h if up else z + h
        inside = source >= 0 if up else source < deep
        more = has_up if up else has_down
        far = above if up else below
        g = slot(y, jnp.clip(source, 0, deep - 1), x)
        sems = fwd_send.at[0 if up else 1, h - 1]

        def arrive(k):
            @pl.when(inside)
            def _():
                landed(q_all.at[span(g), columns(k)], q_recv.at[g, k])

                @pl.when(more)
                def _():
                    pass_on(g, k, sems.at[0], far)

                pass_on(g, k, sems.at[1], across)
                pass_on(g, k, sems.at[2], along)

        waits.append((inside & more, whole, sems.at[0]))
        waits.append((inside, whole, sems.at[1]))
        waits.append((inside, whole, sems.at[2]))
        return arrive

    def corner_step(source, inside, sem):
        at = jnp.clip(source, 0, deep - 1)
        gx, gy = slot(y, at, xn), slot(yn, at, x)

        def forward(k):
            g, to, n = (gx, along, 0) if k % 2 == 0 else (gy, across, 1)

            def go():
                landed(q_all.at[span(g), columns(k)], q_recv.at[g, k])
                pass_on(g, k, sem.at[n], to)

            if inside is None:
                go()
            else:
                pl.when(inside)(go)

        waits.append((inside, q_all.at[span(me), left], sem.at[0]))
        waits.append((inside, q_all.at[span(me), left], sem.at[1]))
        return forward

    corners = [corner_step(z, None, diag_send.at[0, 0])]
    for h in range(1, deep):
        arrivals = [column_step(h, True), column_step(h, False)]
        for k in range(steps):
            for go in arrivals:
                go(k)
            for go in corners:
                go(k)
        if h == 1:
            @pl.when(core == 1)
            def _():
                pl.semaphore_signal(turn_sem, inc=1, device_id=mate, device_id_type=MESH)

        corners = [
            corner_step(z - h, z - h >= 0, diag_send.at[0, h]),
            corner_step(z + h, z + h < deep, diag_send.at[1, h]),
        ]
    for k in range(steps):
        for go in corners:
            go(k)
    landed(p_mate, mate_recv.at[0])
    landed(meta_all.at[yn], meta_recv)

    for k in range(steps):
        for b in range(deep):
            zb = turn(z, b, deep)
            g = slot(yn, zb, x) if k % 2 == 0 else slot(y, zb, xn)
            gd = slot(yn, zb, xn)
            landed(q_all.at[span(g), columns(k)], q_recv.at[g, k])
            landed(q_all.at[span(gd), columns(k)], q_recv.at[gd, k])
        ks = columns(k)
        q_piece = q_all[:, ks]
        for at, p_part in ((0, p_own), (own, p_mate)):
            value = lax.dot_general(
                p_part[:, ks], q_piece, (((1,), (1,)), ((), ())), preferred_element_type=jnp.float32
            )
            if k:
                scores[at : at + own, :] += value
            else:
                scores[at : at + own, :] = value

    mt = jnp.concatenate([meta_all[a] for a in range(rows)], axis=1)
    at = lax.broadcasted_iota(jnp.int32, (2 * own, queries), 0)
    first = ((chip * cores + core) * rows + y) * own
    second = ((chip * cores + (1 - core)) * rows + y) * own
    ids = jnp.where(at < own, at + first, at - own + second).astype(jnp.float32)
    sc = scores[...] * inv_temp
    positive = ids == mt[fields // 2 : fields // 2 + 1, :]
    picked_here = jnp.sum(jnp.where(positive, sc, 0.0), axis=0, keepdims=True)
    kept = positive
    for n in range(negs):
        kept = kept | (ids == mt[n : n + 1, :])
    held_here = jnp.max(jnp.where(kept, sc, -jnp.inf), axis=0, keepdims=True)
    pick_out[...] = jnp.concatenate([picked_here, held_here], axis=1)
    for n, peer in enumerate(peers):
        send(pick_out, pick_all.at[me], pick_send.at[n], pick_recv.at[me], device(*peer))
    pick_all[me] = pick_out[...]
    for peer in peers:
        g = slot(*peer)
        landed(pick_all.at[g], pick_recv.at[g])
    picks = pick_all[...]
    picked = jnp.sum(picks[:, :, :queries], axis=0)
    held = jnp.max(picks[:, :, queries:], axis=0)
    v = sharpness * (sc - picked - mt[fields // 2 + 1 : fields // 2 + 2, :])
    penalty = jnp.maximum(v, 0.0) + jnp.log1p(jnp.exp(-jnp.abs(v)))
    grown = jnp.exp(jnp.where(kept, sc, sc - penalty) - held)
    sum_here = jnp.sum(grown, axis=0, keepdims=True)
    stat_out[...] = sum_here
    for n, peer in enumerate(peers):
        send(stat_out, stat_all.at[me], stat_send.at[n], stat_recv.at[me], device(*peer))
    stat_all[me] = sum_here
    for peer in peers:
        g = slot(*peer)
        landed(stat_all.at[g], stat_recv.at[g])
    total = jnp.sum(stat_all[...], axis=0)
    losses = jnp.broadcast_to(held + jnp.log(total) - picked, (8, queries))
    loss_ref[...] = pltpu.roll(losses, lax.rem(queries - me * block, queries), 1)[:1, :block]
    factor = 1.0 / total
    grad = ((grown * factor - positive.astype(jnp.float32)) * inv_temp).astype(jnp.bfloat16)
    grad_t = jnp.transpose(grad)

    cuts = 8
    cut = depth // cuts
    parts = 4
    share = depth // parts
    per = parts // 2
    mix = [k for pair in zip(range(per), range(per, parts)) for k in pair]
    low_half = z < deep // 2
    folded = jnp.where(low_half, z, deep - 1 - z)

    def target(n):
        if n == deep - 1:
            return z
        v = deep - 1 - n
        v = jnp.where(v > folded, v, v - 1)
        return jnp.where(low_half, v, deep - 1 - v)

    targets = [target(n) for n in range(deep)]

    def area(k, wrap=False):
        return pl.ds((k % per if wrap else k) * share, share)

    def post(src, dst, send_sem, recv_sem, to):
        pltpu.make_async_remote_copy(
            src_ref=src, dst_ref=dst, send_sem=send_sem, recv_sem=recv_sem,
            device_id=to, device_id_type=MESH,
        ).start()

    def route(k):
        return (along, across) if k < per else (across, along)

    def diagonal(n, k):
        gd = slot(yn, targets[n], xn)
        into = diag_in_y if k < per else diag_in_x
        post(
            part_low.at[span(gd), area(k)], into.at[n, :, area(k, True)],
            rd_send.at[n, k // per], rd_recv.at[n, k], route(k)[0],
        )

    def plain(n, k):
        g, into = (slot(yn, targets[n], x), in_y) if k < per else (slot(y, targets[n], xn), in_x)
        post(
            part_low.at[span(g), area(k)], into.at[n, :, area(k)],
            ru_send.at[n, k // per], ru_recv.at[n, k], route(k)[0],
        )

    def merged(n, k):
        g = slot(y, targets[n], xn) if k < per else slot(yn, targets[n], x)
        got, out, into = (diag_in_y, merge_x, in_x) if k < per else (diag_in_x, merge_y, in_y)
        landed(got.at[n, :, area(k, True)], rd_recv.at[n, k])
        out[n, :, area(k, True)] = (
            part[span(g), area(k)] + got[n, :, area(k, True)].astype(jnp.float32)
        ).astype(jnp.bfloat16)
        post(
            out.at[n, :, area(k, True)], into.at[n, :, area(k)],
            rm_send.at[n, k // per], rm_recv.at[n, k], route(k)[1],
        )

    def z_buffers(n):
        return (z_out_full, z_in_full) if n >= deep // 2 else (z_out, z_in)

    def settle(n, k):
        landed((in_y if k < per else in_x).at[n, :, area(k)], ru_recv.at[n, k])
        landed((in_x if k < per else in_y).at[n, :, area(k)], rm_recv.at[n, k])
        g = slot(y, targets[n], x)
        value = (
            part[span(g), area(k)]
            + in_x[n, :, area(k)].astype(jnp.float32)
            + in_y[n, :, area(k)].astype(jnp.float32)
        )
        if n < deep - 1:
            out, into = z_buffers(n)
            out[n, :, area(k)] = value.astype(out.dtype)
            post(
                out.at[n, :, area(k)], into.at[z, :, area(k)],
                z_send.at[n], z_recv.at[z, k], device(y, targets[n], x),
            )
        else:
            plane[:, area(k)] = value

    for k in mix:
        value = jnp.dot(grad_t[:, :own], p_own[:, area(k)], preferred_element_type=jnp.float32) + jnp.dot(
            grad_t[:, own:], p_mate[:, area(k)], preferred_element_type=jnp.float32
        )
        part[:, area(k)] = value
        part_low[:, area(k)] = value.astype(jnp.bfloat16)
        diagonal(0, k)
    for k in mix:
        diagonal(1, k)
    for k in mix:
        plain(0, k)

    @pl.loop(0, cuts)
    def _(k):
        ks = pl.ds(pl.multiple_of(k * cut, lane), cut)
        gp_out[:, ks] = jnp.dot(grad[own:, :], q_all[:, ks], preferred_element_type=jnp.float32)

    send(gp_out, gp_in, mate_send.at[1], mate_recv.at[1], mate)

    for n in range(deep):
        for k in mix:
            merged(n, k)
            if n + 2 < deep:
                diagonal(n + 2, k)
        if n + 1 < deep:
            for k in mix:
                plain(n + 1, k)
        if n:
            for k in mix:
                settle(n - 1, k)

    landed(gp_in, mate_recv.at[1])

    @pl.loop(0, cuts)
    def _(k):
        ks = pl.ds(pl.multiple_of(k * cut, lane), cut)
        gp_ref[:, ks] = (
            jnp.dot(grad[:own, :], q_all[:, ks], preferred_element_type=jnp.float32) + gp_in[:, ks]
        )

    for k in mix:
        settle(deep - 1, k)
        value = plane[:, area(k)]
        for n in range(deep - 1):
            into = z_buffers(n)[1]
            landed(into.at[targets[n], :, area(k)], z_recv.at[targets[n], k])
            value = value + into[targets[n], :, area(k)].astype(jnp.float32)
        gq_ref[:, area(k)] = value
    for n in range(deep):
        for side in range(2):
            for sem in (rd_send, ru_send, rm_send):
                waits.append((None, merge_x.at[n], sem.at[n, side]))
        if n < deep - 1:
            waits.append((None, z_buffers(n)[0].at[n], z_send.at[n]))
    for inside, ref, sem in waits:
        if inside is None:
            landed(ref, sem)
        else:
            pl.when(inside)(functools.partial(landed, ref, sem))
    for copy in sent:
        copy.wait_send()


def store_kernel(loss_ref, gq_ref, gp_ref, loss_out, gq_out, gp_out, sems):
    copies = [
        pltpu.make_async_copy(source, out, sems.at[n])
        for n, (source, out) in enumerate(((gp_ref, gp_out), (gq_ref, gq_out), (loss_ref, loss_out)))
    ]
    for copy in copies:
        copy.start()
    for copy in copies:
        copy.wait()


def on_device(queries, passages, positives, hard_negatives, thresholds):
    rows, columns = lax.axis_size("row"), lax.axis_size("col")
    wide = rows
    deep = columns // (cores * wide)
    block, depth = queries.shape
    own = passages.shape[0]
    negs = hard_negatives.shape[1]
    run = deep * wide * block
    fits = rows == 2 and columns % (cores * wide) == 0 and deep > 1 and deep % 2 == 0
    fits = fits and block % 16 == 0 and run % lane == 0 and negs <= fields // 2 and depth % 1024 == 0
    if not fits:
        return general_plan(queries, passages, positives, hard_negatives, thresholds)
    groups = rows * deep * wide
    total = groups * block
    half = depth // 2
    low, full = jnp.bfloat16, jnp.float32
    dma = pltpu.SemaphoreType.DMA
    results = pl.pallas_call(
        functools.partial(step_kernel, rows, wide, deep, negs),
        out_shape=(
            jax.ShapeDtypeStruct((1, block), full),
            jax.ShapeDtypeStruct((block, depth), full),
            jax.ShapeDtypeStruct((own, depth), full),
        ),
        in_specs=[pl.BlockSpec(memory_space=pltpu.HBM)] * 5,
        out_specs=[pl.BlockSpec(memory_space=pltpu.VMEM)] * 3,
        scratch_shapes=[
            pltpu.VMEM((own, depth), low),
            pltpu.VMEM((1, positives.shape[0]), jnp.int32),
            pltpu.VMEM((negs, positives.shape[0]), jnp.int32),
            pltpu.VMEM((1, positives.shape[0]), full),
            pltpu.VMEM((total, depth), low),
            pltpu.VMEM((own, depth), low),
            pltpu.VMEM((lane, columns * block), full),
            pltpu.VMEM((fields, run), full),
            pltpu.VMEM((rows, fields, run), full),
            pltpu.VMEM((cores * own, total), full),
            pltpu.VMEM((1, 2 * total), full),
            pltpu.VMEM((groups, 1, 2 * total), full),
            pltpu.VMEM((1, total), full),
            pltpu.VMEM((groups, 1, total), full),
            pltpu.VMEM((total, depth), full),
            pltpu.VMEM((total, depth), low),
            pltpu.VMEM((own, depth), full),
            pltpu.VMEM((own, depth), full),
            pltpu.VMEM((deep, block, half), low),
            pltpu.VMEM((deep, block, half), low),
            pltpu.VMEM((deep, block, half), low),
            pltpu.VMEM((deep, block, half), low),
            pltpu.VMEM((deep, block, depth), low),
            pltpu.VMEM((deep, block, depth), low),
            pltpu.VMEM((block, depth), full),
            pltpu.VMEM((deep, block, depth), low),
            pltpu.VMEM((deep, block, depth), low),
            pltpu.VMEM((deep, block, depth), full),
            pltpu.VMEM((deep, block, depth), full),
            dma((5,)), dma((4,)), dma((2, deep, 3)), dma((2, deep, 2)), dma((groups, 4)),
            dma((2,)), dma((2,)), dma, dma,
            dma((groups,)), dma((groups,)), dma((groups,)), dma((groups,)),
            dma((deep, 2)), dma((deep, 4)), dma((deep, 2)), dma((deep, 4)),
            dma((deep, 2)), dma((deep, 4)), dma((deep,)), dma((deep, 4)),
            pltpu.SemaphoreType.REGULAR,
        ],
        compiler_params=pltpu.CompilerParams(
            collective_id=0, has_side_effects=True, vmem_limit_bytes=44 * 1024 * 1024
        ),
    )(*(
        pltpu.with_memory_space_constraint(a, pltpu.HBM)
        for a in (queries, passages, positives[None], hard_negatives.T, thresholds[None])
    ))
    losses, grad_queries, grad_passages = pl.pallas_call(
        store_kernel,
        out_shape=[jax.ShapeDtypeStruct(a.shape, a.dtype) for a in results],
        in_specs=[pl.BlockSpec(memory_space=pltpu.VMEM)] * 3,
        out_specs=[pl.BlockSpec(memory_space=pltpu.HBM)] * 3,
        scratch_shapes=[dma((3,))],
        compiler_params=pltpu.CompilerParams(vmem_limit_bytes=8 * 1024 * 1024),
    )(*results)
    return (losses[0], grad_queries, grad_passages)


def solution(mesh):
    placed = (P(("row", "col"), None), P(("col", "row"), None), P("row"), P("row", None), P("row"))
    return jax.shard_map(
        on_device,
        mesh=mesh,
        in_specs=placed,
        out_specs=(P(("row", "col")), P(("row", "col"), None), P(("col", "row"), None)),
        check_vma=False,
    )
```

```python
import functools
import jax
import jax.numpy as jnp
from jax import lax
from jax.experimental import pallas as pl
from jax.experimental.pallas import tpu as pltpu
from jax.sharding import PartitionSpec as P

inv_temp = 50.0
sharpness = 4.0


def combined_all(part, axis, combine):
    gathered = jax.tree.map(lambda a: lax.all_gather(a, axis), part)

    def take(source):
        return jax.tree.map(lambda a: lax.dynamic_index_in_dim(a, source, 0, False), gathered)

    return lax.fori_loop(
        1, lax.axis_size(axis), lambda source, state: combine(state, take(source)), take(0)
    )


def pair_merge(left_pair, right_pair):
    left_top, left_total = left_pair
    right_top, right_total = right_pair
    joined = jnp.maximum(left_top, right_top)
    return (
        joined,
        left_total * jnp.exp(left_top - joined) + right_total * jnp.exp(right_top - joined),
    )


def general_plan(queries, passages, positives, hard_negatives, thresholds):
    query_block = lax.all_gather(queries, "col", axis=0, tiled=True)
    passage_block = lax.all_gather(passages, "row", axis=0, tiled=True)
    block_width = passage_block.shape[0]
    query_rows = queries.shape[0]
    scores = jnp.dot(query_block, passage_block.T, preferred_element_type=jnp.float32) * inv_temp
    columns = lax.axis_index("col") * block_width + lax.iota(jnp.int32, block_width)
    positive_mask = positives[:, None] == columns[None, :]
    kept_mask = positive_mask
    for mined_slot in range(hard_negatives.shape[1]):
        kept_mask = kept_mask | (hard_negatives[:, mined_slot : mined_slot + 1] == columns[None, :])
    picked = lax.psum(jnp.sum(jnp.where(positive_mask, scores, 0.0), axis=1), "col")
    penalty = jax.nn.softplus(sharpness * (scores - picked[:, None] - thresholds[:, None]))
    logits = jnp.where(kept_mask, scores, scores - penalty)
    local_top = jnp.max(logits, axis=1)
    local_exp = jnp.exp(logits - local_top[:, None])
    row_top, denominator = combined_all((local_top, jnp.sum(local_exp, axis=1)), "col", pair_merge)
    shifted = local_exp * jnp.exp(local_top - row_top)[:, None]
    losses = row_top + jnp.log(denominator) - picked
    row_losses = lax.dynamic_slice_in_dim(losses, lax.axis_index("col") * query_rows, query_rows, 0)
    grad_scores = (
        (shifted / denominator[:, None] - positive_mask.astype(jnp.float32)) * inv_temp
    ).astype(jnp.bfloat16)
    query_full = jnp.dot(grad_scores, passage_block, preferred_element_type=jnp.float32)
    grad_queries = lax.psum_scatter(query_full, "col", scatter_dimension=0, tiled=True)
    passage_full = lax.dot_general(
        grad_scores, query_block, (((0,), (0,)), ((), ())), preferred_element_type=jnp.float32
    )
    grad_passages = lax.psum_scatter(passage_full, "row", scatter_dimension=0, tiled=True)
    return (row_losses, grad_queries, grad_passages)


cores = 2
lane = 128
fields = 16
MESH = pl.DeviceIdType.MESH


def step_kernel(
    rows, wide, deep, negs,
    q_ref, p_ref, positives_ref, mined_ref, thresholds_ref,
    loss_ref, gq_ref, gp_ref,
    p_own, positives_own, mined_own, thresholds_own,
    q_all, p_mate, mined_wide, meta_ref, meta_all, scores, pick_out, pick_all, stat_out, stat_all,
    part, part_low, gp_out, gp_in,
    diag_in_y, diag_in_x, merge_x, merge_y, in_x, in_y, plane, z_out, z_in, z_out_full, z_in_full,
    load_sem, own_send, fwd_send, diag_send, q_recv,
    mate_send, mate_recv, meta_send, meta_recv,
    pick_send, pick_recv, stat_send, stat_recv,
    rd_send, rd_recv, ru_send, ru_recv, rm_send, rm_recv, z_send, z_recv, turn_sem,
):
    y = lax.axis_index("row")
    col = lax.axis_index("col")
    core = lax.rem(col, cores)
    chip = col // cores
    z = chip // wide
    x = lax.rem(chip, wide)
    block, depth = q_ref.shape
    half = depth // 2
    own = p_ref.shape[0]
    groups = rows * deep * wide
    queries = groups * block

    def device(yy, zz, xx, cc=None):
        return (yy, (zz * wide + xx) * cores + (core if cc is None else cc))

    def slot(yy, zz, xx):
        return (yy * deep + zz) * wide + xx

    def span(g):
        return pl.ds(pl.multiple_of(g * block, block), block)

    def turn(at, by, size):
        return lax.rem(at + by, size)

    def send(src, dst, send_sem, recv_sem, to):
        copy = pltpu.make_async_remote_copy(
            src_ref=src, dst_ref=dst, send_sem=send_sem, recv_sem=recv_sem,
            device_id=to, device_id_type=MESH,
        )
        copy.start()
        sent.append(copy)

    def landed(ref, sem):
        pltpu.make_async_copy(ref, ref, sem).wait()

    sent = []
    waits = []
    left, right = pl.ds(0, half), pl.ds(half, half)
    yn, xn = turn(y, 1, rows), turn(x, 1, wide)
    me = slot(y, z, x)
    mate = device(y, z, x, 1 - core)
    across, along = device(y, z, xn), device(yn, z, x)
    peers = [
        (turn(y, a, rows), turn(z, b, deep), turn(x, d, wide))
        for b in range(deep) for a in range(rows) for d in range(wide) if a + b + d
    ]
    steps = 4
    width = depth // steps

    def columns(k):
        return pl.ds(k * width, width)

    q_load = pltpu.make_async_copy(q_ref, q_all.at[span(me)], load_sem.at[0])
    p_load = pltpu.make_async_copy(p_ref, p_own, load_sem.at[1])
    tables = [
        pltpu.make_async_copy(positives_ref, positives_own, load_sem.at[2]),
        pltpu.make_async_copy(mined_ref, mined_own, load_sem.at[3]),
        pltpu.make_async_copy(thresholds_ref, thresholds_own, load_sem.at[4]),
    ]
    q_load.start()
    p_load.start()
    for table in tables:
        table.start()

    has_up, has_down = z < deep - 1, z > 0
    above = device(y, jnp.minimum(z + 1, deep - 1), x)
    below = device(y, jnp.maximum(z - 1, 0), x)
    barrier = pltpu.get_barrier_semaphore()
    for to in (across, along, mate):
        pl.semaphore_signal(barrier, inc=1, device_id=to, device_id_type=MESH)

    @pl.when(has_up)
    def _():
        pl.semaphore_signal(barrier, inc=1, device_id=above, device_id_type=MESH)

    @pl.when(has_down)
    def _():
        pl.semaphore_signal(barrier, inc=1, device_id=below, device_id_type=MESH)

    pl.semaphore_wait(barrier, 3 + jnp.where(has_up, 1, 0) + jnp.where(has_down, 1, 0))
    q_load.wait()

    def pass_on(g, k, sem, to):
        ref = q_all.at[span(g), columns(k)]
        pltpu.make_async_remote_copy(
            src_ref=ref, dst_ref=ref, send_sem=sem, recv_sem=q_recv.at[g, k],
            device_id=to, device_id_type=MESH,
        ).start()

    whole = q_all.at[span(me)]

    @pl.when(core == 0)
    def _():
        pl.semaphore_wait(turn_sem, 1)

    for k in range(steps):
        @pl.when(has_up)
        def _():
            pass_on(me, k, own_send.at[0], above)

        @pl.when(has_down)
        def _():
            pass_on(me, k, own_send.at[1], below)

        pass_on(me, k, own_send.at[2], across)
        pass_on(me, k, own_send.at[3], along)
    waits.append((has_up, whole, own_send.at[0]))
    waits.append((has_down, whole, own_send.at[1]))
    waits.append((None, whole, own_send.at[2]))
    waits.append((None, whole, own_send.at[3]))
    p_load.wait()
    send(p_own, p_mate, mate_send.at[0], mate_recv.at[0], mate)
    for table in tables:
        table.wait()

    def mine(table):
        return jnp.concatenate(
            [table[(m * cores) * block : (m * cores + 1) * block] for m in range(deep * wide)], axis=0
        ), jnp.concatenate(
            [table[(m * cores + 1) * block : (m * cores + 2) * block] for m in range(deep * wide)], axis=0
        )

    mined_wide[...] = jnp.zeros_like(mined_wide)
    mined_wide[:negs, :] = mined_own[...].astype(jnp.float32)
    mined_wide[fields // 2 : fields // 2 + 1, :] = positives_own[...].astype(jnp.float32)
    mined_wide[fields // 2 + 1 : fields // 2 + 2, :] = thresholds_own[...]
    one_first, one_second = mine(jnp.transpose(mined_wide[...]))
    meta_ref[...] = jnp.transpose(jnp.where(core == 0, one_first, one_second))[:fields]
    meta_all[y] = meta_ref[...]
    send(meta_ref, meta_all.at[y], meta_send, meta_recv, device(yn, z, x))

    def column_step(h, up):
        source = z - h if up else z + h
        inside = source >= 0 if up else source < deep
        more = has_up if up else has_down
        far = above if up else below
        g = slot(y, jnp.clip(source, 0, deep - 1), x)
        sems = fwd_send.at[0 if up else 1, h - 1]

        def arrive(k):
            @pl.when(inside)
            def _():
                landed(q_all.at[span(g), columns(k)], q_recv.at[g, k])

                @pl.when(more)
                def _():
                    pass_on(g, k, sems.at[0], far)

                pass_on(g, k, sems.at[1], across)
                pass_on(g, k, sems.at[2], along)

        waits.append((inside & more, whole, sems.at[0]))
        waits.append((inside, whole, sems.at[1]))
        waits.append((inside, whole, sems.at[2]))
        return arrive

    def corner_step(source, inside, sem):
        at = jnp.clip(source, 0, deep - 1)
        gx, gy = slot(y, at, xn), slot(yn, at, x)

        def forward(k):
            g, to, n = (gx, along, 0) if k % 2 == 0 else (gy, across, 1)

            def go():
                landed(q_all.at[span(g), columns(k)], q_recv.at[g, k])
                pass_on(g, k, sem.at[n], to)

            if inside is None:
                go()
            else:
                pl.when(inside)(go)

        waits.append((inside, q_all.at[span(me), left], sem.at[0]))
        waits.append((inside, q_all.at[span(me), left], sem.at[1]))
        return forward

    corners = [corner_step(z, None, diag_send.at[0, 0])]
    for h in range(1, deep):
        arrivals = [column_step(h, True), column_step(h, False)]
        for k in range(steps):
            for go in arrivals:
                go(k)
            for go in corners:
                go(k)
        if h == 1:
            @pl.when(core == 1)
            def _():
                pl.semaphore_signal(turn_sem, inc=1, device_id=mate, device_id_type=MESH)

        corners = [
            corner_step(z - h, z - h >= 0, diag_send.at[0, h]),
            corner_step(z + h, z + h < deep, diag_send.at[1, h]),
        ]
    for k in range(steps):
        for go in corners:
            go(k)
    landed(p_mate, mate_recv.at[0])
    landed(meta_all.at[yn], meta_recv)

    for k in range(steps):
        for b in range(deep):
            zb = turn(z, b, deep)
            g = slot(yn, zb, x) if k % 2 == 0 else slot(y, zb, xn)
            gd = slot(yn, zb, xn)
            landed(q_all.at[span(g), columns(k)], q_recv.at[g, k])
            landed(q_all.at[span(gd), columns(k)], q_recv.at[gd, k])
        ks = columns(k)
        q_piece = q_all[:, ks]
        for at, p_part in ((0, p_own), (own, p_mate)):
            value = lax.dot_general(
                p_part[:, ks], q_piece, (((1,), (1,)), ((), ())), preferred_element_type=jnp.float32
            )
            if k:
                scores[at : at + own, :] += value
            else:
                scores[at : at + own, :] = value

    mt = jnp.concatenate([meta_all[a] for a in range(rows)], axis=1)
    at = lax.broadcasted_iota(jnp.int32, (2 * own, queries), 0)
    first = ((chip * cores + core) * rows + y) * own
    second = ((chip * cores + (1 - core)) * rows + y) * own
    ids = jnp.where(at < own, at + first, at - own + second).astype(jnp.float32)
    sc = scores[...] * inv_temp
    positive = ids == mt[fields // 2 : fields // 2 + 1, :]
    picked_here = jnp.sum(jnp.where(positive, sc, 0.0), axis=0, keepdims=True)
    kept = positive
    for n in range(negs):
        kept = kept | (ids == mt[n : n + 1, :])
    held_here = jnp.max(jnp.where(kept, sc, -jnp.inf), axis=0, keepdims=True)
    pick_out[...] = jnp.concatenate([picked_here, held_here], axis=1)
    for n, peer in enumerate(peers):
        send(pick_out, pick_all.at[me], pick_send.at[n], pick_recv.at[me], device(*peer))
    pick_all[me] = pick_out[...]
    for peer in peers:
        g = slot(*peer)
        landed(pick_all.at[g], pick_recv.at[g])
    picks = pick_all[...]
    picked = jnp.sum(picks[:, :, :queries], axis=0)
    held = jnp.max(picks[:, :, queries:], axis=0)
    v = sharpness * (sc - picked - mt[fields // 2 + 1 : fields // 2 + 2, :])
    penalty = jnp.maximum(v, 0.0) + jnp.log1p(jnp.exp(-jnp.abs(v)))
    grown = jnp.exp(jnp.where(kept, sc, sc - penalty) - held)
    sum_here = jnp.sum(grown, axis=0, keepdims=True)
    stat_out[...] = sum_here
    for n, peer in enumerate(peers):
        send(stat_out, stat_all.at[me], stat_send.at[n], stat_recv.at[me], device(*peer))
    stat_all[me] = sum_here
    for peer in peers:
        g = slot(*peer)
        landed(stat_all.at[g], stat_recv.at[g])
    total = jnp.sum(stat_all[...], axis=0)
    losses = jnp.broadcast_to(held + jnp.log(total) - picked, (8, queries))
    loss_ref[...] = pltpu.roll(losses, lax.rem(queries - me * block, queries), 1)[:1, :block]
    factor = 1.0 / total
    grad = ((grown * factor - positive.astype(jnp.float32)) * inv_temp).astype(jnp.bfloat16)
    grad_t = jnp.transpose(grad)

    cuts = 8
    cut = depth // cuts
    parts = 4
    share = depth // parts
    per = parts // 2
    mix = [k for pair in zip(range(per), range(per, parts)) for k in pair]
    low_half = z < deep // 2
    folded = jnp.where(low_half, z, deep - 1 - z)

    def target(n):
        if n == deep - 1:
            return z
        v = deep - 1 - n
        v = jnp.where(v > folded, v, v - 1)
        return jnp.where(low_half, v, deep - 1 - v)

    targets = [target(n) for n in range(deep)]

    def area(k, wrap=False):
        return pl.ds((k % per if wrap else k) * share, share)

    def post(src, dst, send_sem, recv_sem, to):
        pltpu.make_async_remote_copy(
            src_ref=src, dst_ref=dst, send_sem=send_sem, recv_sem=recv_sem,
            device_id=to, device_id_type=MESH,
        ).start()

    def route(k):
        return (along, across) if k < per else (across, along)

    def diagonal(n, k):
        gd = slot(yn, targets[n], xn)
        into = diag_in_y if k < per else diag_in_x
        post(
            part_low.at[span(gd), area(k)], into.at[n, :, area(k, True)],
            rd_send.at[n, k // per], rd_recv.at[n, k], route(k)[0],
        )

    def plain(n, k):
        g, into = (slot(yn, targets[n], x), in_y) if k < per else (slot(y, targets[n], xn), in_x)
        post(
            part_low.at[span(g), area(k)], into.at[n, :, area(k)],
            ru_send.at[n, k // per], ru_recv.at[n, k], route(k)[0],
        )

    def merged(n, k):
        g = slot(y, targets[n], xn) if k < per else slot(yn, targets[n], x)
        got, out, into = (diag_in_y, merge_x, in_x) if k < per else (diag_in_x, merge_y, in_y)
        landed(got.at[n, :, area(k, True)], rd_recv.at[n, k])
        out[n, :, area(k, True)] = (
            part[span(g), area(k)] + got[n, :, area(k, True)].astype(jnp.float32)
        ).astype(jnp.bfloat16)
        post(
            out.at[n, :, area(k, True)], into.at[n, :, area(k)],
            rm_send.at[n, k // per], rm_recv.at[n, k], route(k)[1],
        )

    def z_buffers(n):
        return (z_out_full, z_in_full) if n >= deep else (z_out, z_in)

    def settle(n, k):
        landed((in_y if k < per else in_x).at[n, :, area(k)], ru_recv.at[n, k])
        landed((in_x if k < per else in_y).at[n, :, area(k)], rm_recv.at[n, k])
        g = slot(y, targets[n], x)
        value = (
            part[span(g), area(k)]
            + in_x[n, :, area(k)].astype(jnp.float32)
            + in_y[n, :, area(k)].astype(jnp.float32)
        )
        if n < deep - 1:
            out, into = z_buffers(n)
            out[n, :, area(k)] = value.astype(out.dtype)
            post(
                out.at[n, :, area(k)], into.at[z, :, area(k)],
                z_send.at[n], z_recv.at[z, k], device(y, targets[n], x),
            )
        else:
            plane[:, area(k)] = value

    for k in mix:
        value = jnp.dot(grad_t[:, :own], p_own[:, area(k)], preferred_element_type=jnp.float32) + jnp.dot(
            grad_t[:, own:], p_mate[:, area(k)], preferred_element_type=jnp.float32
        )
        part[:, area(k)] = value
        part_low[:, area(k)] = value.astype(jnp.bfloat16)
        diagonal(0, k)
    for k in mix:
        diagonal(1, k)
    for k in mix:
        plain(0, k)

    @pl.loop(0, cuts)
    def _(k):
        ks = pl.ds(pl.multiple_of(k * cut, lane), cut)
        gp_out[:, ks] = jnp.dot(grad[own:, :], q_all[:, ks], preferred_element_type=jnp.float32)

    send(gp_out, gp_in, mate_send.at[1], mate_recv.at[1], mate)

    for n in range(deep):
        for k in mix:
            merged(n, k)
            if n + 2 < deep:
                diagonal(n + 2, k)
        if n + 1 < deep:
            for k in mix:
                plain(n + 1, k)
        if n:
            for k in mix:
                settle(n - 1, k)

    landed(gp_in, mate_recv.at[1])

    @pl.loop(0, cuts)
    def _(k):
        ks = pl.ds(pl.multiple_of(k * cut, lane), cut)
        gp_ref[:, ks] = (
            jnp.dot(grad[:own, :], q_all[:, ks], preferred_element_type=jnp.float32) + gp_in[:, ks]
        )

    for k in mix:
        settle(deep - 1, k)
        value = plane[:, area(k)]
        for n in range(deep - 1):
            into = z_buffers(n)[1]
            landed(into.at[targets[n], :, area(k)], z_recv.at[targets[n], k])
            value = value + into[targets[n], :, area(k)].astype(jnp.float32)
        gq_ref[:, area(k)] = value
    for n in range(deep):
        for side in range(2):
            for sem in (rd_send, ru_send, rm_send):
                waits.append((None, merge_x.at[n], sem.at[n, side]))
        if n < deep - 1:
            waits.append((None, z_buffers(n)[0].at[n], z_send.at[n]))
    for inside, ref, sem in waits:
        if inside is None:
            landed(ref, sem)
        else:
            pl.when(inside)(functools.partial(landed, ref, sem))
    for copy in sent:
        copy.wait_send()


def store_kernel(loss_ref, gq_ref, gp_ref, loss_out, gq_out, gp_out, sems):
    copies = [
        pltpu.make_async_copy(source, out, sems.at[n])
        for n, (source, out) in enumerate(((gp_ref, gp_out), (gq_ref, gq_out), (loss_ref, loss_out)))
    ]
    for copy in copies:
        copy.start()
    for copy in copies:
        copy.wait()


def on_device(queries, passages, positives, hard_negatives, thresholds):
    rows, columns = lax.axis_size("row"), lax.axis_size("col")
    wide = rows
    deep = columns // (cores * wide)
    block, depth = queries.shape
    own = passages.shape[0]
    negs = hard_negatives.shape[1]
    run = deep * wide * block
    fits = rows == 2 and columns % (cores * wide) == 0 and deep > 1 and deep % 2 == 0
    fits = fits and block % 16 == 0 and run % lane == 0 and negs <= fields // 2 and depth % 1024 == 0
    if not fits:
        return general_plan(queries, passages, positives, hard_negatives, thresholds)
    groups = rows * deep * wide
    total = groups * block
    half = depth // 2
    low, full = jnp.bfloat16, jnp.float32
    dma = pltpu.SemaphoreType.DMA
    results = pl.pallas_call(
        functools.partial(step_kernel, rows, wide, deep, negs),
        out_shape=(
            jax.ShapeDtypeStruct((1, block), full),
            jax.ShapeDtypeStruct((block, depth), full),
            jax.ShapeDtypeStruct((own, depth), full),
        ),
        in_specs=[pl.BlockSpec(memory_space=pltpu.HBM)] * 5,
        out_specs=[pl.BlockSpec(memory_space=pltpu.VMEM)] * 3,
        scratch_shapes=[
            pltpu.VMEM((own, depth), low),
            pltpu.VMEM((1, positives.shape[0]), jnp.int32),
            pltpu.VMEM((negs, positives.shape[0]), jnp.int32),
            pltpu.VMEM((1, positives.shape[0]), full),
            pltpu.VMEM((total, depth), low),
            pltpu.VMEM((own, depth), low),
            pltpu.VMEM((lane, columns * block), full),
            pltpu.VMEM((fields, run), full),
            pltpu.VMEM((rows, fields, run), full),
            pltpu.VMEM((cores * own, total), full),
            pltpu.VMEM((1, 2 * total), full),
            pltpu.VMEM((groups, 1, 2 * total), full),
            pltpu.VMEM((1, total), full),
            pltpu.VMEM((groups, 1, total), full),
            pltpu.VMEM((total, depth), full),
            pltpu.VMEM((total, depth), low),
            pltpu.VMEM((own, depth), full),
            pltpu.VMEM((own, depth), full),
            pltpu.VMEM((deep, block, half), low),
            pltpu.VMEM((deep, block, half), low),
            pltpu.VMEM((deep, block, half), low),
            pltpu.VMEM((deep, block, half), low),
            pltpu.VMEM((deep, block, depth), low),
            pltpu.VMEM((deep, block, depth), low),
            pltpu.VMEM((block, depth), full),
            pltpu.VMEM((deep, block, depth), low),
            pltpu.VMEM((deep, block, depth), low),
            pltpu.VMEM((deep, block, depth), full),
            pltpu.VMEM((deep, block, depth), full),
            dma((5,)), dma((4,)), dma((2, deep, 3)), dma((2, deep, 2)), dma((groups, 4)),
            dma((2,)), dma((2,)), dma, dma,
            dma((groups,)), dma((groups,)), dma((groups,)), dma((groups,)),
            dma((deep, 2)), dma((deep, 4)), dma((deep, 2)), dma((deep, 4)),
            dma((deep, 2)), dma((deep, 4)), dma((deep,)), dma((deep, 4)),
            pltpu.SemaphoreType.REGULAR,
        ],
        compiler_params=pltpu.CompilerParams(
            collective_id=0, has_side_effects=True, vmem_limit_bytes=44 * 1024 * 1024
        ),
    )(*(
        pltpu.with_memory_space_constraint(a, pltpu.HBM)
        for a in (queries, passages, positives[None], hard_negatives.T, thresholds[None])
    ))
    losses, grad_queries, grad_passages = pl.pallas_call(
        store_kernel,
        out_shape=[jax.ShapeDtypeStruct(a.shape, a.dtype) for a in results],
        in_specs=[pl.BlockSpec(memory_space=pltpu.VMEM)] * 3,
        out_specs=[pl.BlockSpec(memory_space=pltpu.HBM)] * 3,
        scratch_shapes=[dma((3,))],
        compiler_params=pltpu.CompilerParams(vmem_limit_bytes=8 * 1024 * 1024),
    )(*results)
    return (losses[0], grad_queries, grad_passages)


def solution(mesh):
    placed = (P(("row", "col"), None), P(("col", "row"), None), P("row"), P("row", None), P("row"))
    return jax.shard_map(
        on_device,
        mesh=mesh,
        in_specs=placed,
        out_specs=(P(("row", "col")), P(("row", "col"), None), P(("col", "row"), None)),
        check_vma=False,
    )
```

```python
import functools
import jax
import jax.numpy as jnp
from jax import lax
from jax.experimental import pallas as pl
from jax.experimental.pallas import tpu as pltpu
from jax.sharding import PartitionSpec as P

inv_temp = 50.0
sharpness = 4.0


def combined_all(part, axis, combine):
    gathered = jax.tree.map(lambda a: lax.all_gather(a, axis), part)

    def take(source):
        return jax.tree.map(lambda a: lax.dynamic_index_in_dim(a, source, 0, False), gathered)

    return lax.fori_loop(
        1, lax.axis_size(axis), lambda source, state: combine(state, take(source)), take(0)
    )


def pair_merge(left_pair, right_pair):
    left_top, left_total = left_pair
    right_top, right_total = right_pair
    joined = jnp.maximum(left_top, right_top)
    return (
        joined,
        left_total * jnp.exp(left_top - joined) + right_total * jnp.exp(right_top - joined),
    )


def general_plan(queries, passages, positives, hard_negatives, thresholds):
    query_block = lax.all_gather(queries, "col", axis=0, tiled=True)
    passage_block = lax.all_gather(passages, "row", axis=0, tiled=True)
    block_width = passage_block.shape[0]
    query_rows = queries.shape[0]
    scores = jnp.dot(query_block, passage_block.T, preferred_element_type=jnp.float32) * inv_temp
    columns = lax.axis_index("col") * block_width + lax.iota(jnp.int32, block_width)
    positive_mask = positives[:, None] == columns[None, :]
    kept_mask = positive_mask
    for mined_slot in range(hard_negatives.shape[1]):
        kept_mask = kept_mask | (hard_negatives[:, mined_slot : mined_slot + 1] == columns[None, :])
    picked = lax.psum(jnp.sum(jnp.where(positive_mask, scores, 0.0), axis=1), "col")
    penalty = jax.nn.softplus(sharpness * (scores - picked[:, None] - thresholds[:, None]))
    logits = jnp.where(kept_mask, scores, scores - penalty)
    local_top = jnp.max(logits, axis=1)
    local_exp = jnp.exp(logits - local_top[:, None])
    row_top, denominator = combined_all((local_top, jnp.sum(local_exp, axis=1)), "col", pair_merge)
    shifted = local_exp * jnp.exp(local_top - row_top)[:, None]
    losses = row_top + jnp.log(denominator) - picked
    row_losses = lax.dynamic_slice_in_dim(losses, lax.axis_index("col") * query_rows, query_rows, 0)
    grad_scores = (
        (shifted / denominator[:, None] - positive_mask.astype(jnp.float32)) * inv_temp
    ).astype(jnp.bfloat16)
    query_full = jnp.dot(grad_scores, passage_block, preferred_element_type=jnp.float32)
    grad_queries = lax.psum_scatter(query_full, "col", scatter_dimension=0, tiled=True)
    passage_full = lax.dot_general(
        grad_scores, query_block, (((0,), (0,)), ((), ())), preferred_element_type=jnp.float32
    )
    grad_passages = lax.psum_scatter(passage_full, "row", scatter_dimension=0, tiled=True)
    return (row_losses, grad_queries, grad_passages)


cores = 2
lane = 128
fields = 16
MESH = pl.DeviceIdType.MESH


def step_kernel(
    rows, wide, deep, negs,
    q_ref, p_ref, positives_ref, mined_ref, thresholds_ref,
    loss_ref, gq_ref, gp_ref,
    positive_mask, kept_mask, margin, grown_t, positive_t, p_own, positives_own, mined_own, thresholds_own,
    q_all, p_mate, mined_wide, meta_ref, meta_all, scores, pick_out, pick_all, stat_out, stat_all,
    part, part_low, gp_out, gp_in,
    diag_in_y, diag_in_x, merge_x, merge_y, in_x, in_y, plane, z_out, z_in, z_out_full, z_in_full,
    load_sem, own_send, fwd_send, diag_send, q_recv,
    mate_send, mate_recv, meta_send, meta_recv,
    pick_send, pick_recv, stat_send, stat_recv,
    rd_send, rd_recv, ru_send, ru_recv, rm_send, rm_recv, z_send, z_recv, turn_sem,
):
    y = lax.axis_index("row")
    col = lax.axis_index("col")
    core = lax.rem(col, cores)
    chip = col // cores
    z = chip // wide
    x = lax.rem(chip, wide)
    block, depth = q_ref.shape
    half = depth // 2
    own = p_ref.shape[0]
    groups = rows * deep * wide
    queries = groups * block

    def device(yy, zz, xx, cc=None):
        return (yy, (zz * wide + xx) * cores + (core if cc is None else cc))

    def slot(yy, zz, xx):
        return (yy * deep + zz) * wide + xx

    def span(g):
        return pl.ds(pl.multiple_of(g * block, block), block)

    def turn(at, by, size):
        return lax.rem(at + by, size)

    def send(src, dst, send_sem, recv_sem, to):
        copy = pltpu.make_async_remote_copy(
            src_ref=src, dst_ref=dst, send_sem=send_sem, recv_sem=recv_sem,
            device_id=to, device_id_type=MESH,
        )
        copy.start()
        sent.append(copy)

    def landed(ref, sem):
        pltpu.make_async_copy(ref, ref, sem).wait()

    sent = []
    waits = []
    left, right = pl.ds(0, half), pl.ds(half, half)
    yn, xn = turn(y, 1, rows), turn(x, 1, wide)
    me = slot(y, z, x)
    mate = device(y, z, x, 1 - core)
    across, along = device(y, z, xn), device(yn, z, x)
    low_half = z < deep // 2
    folded = jnp.where(low_half, z, deep - 1 - z)

    def target(n):
        if n == deep - 1:
            return z
        v = deep - 1 - n
        v = jnp.where(v > folded, v, v - 1)
        return jnp.where(low_half, v, deep - 1 - v)

    targets = [target(n) for n in range(deep)]

    peers = [
        (yy, zz, xx)
        for n, zz in enumerate(targets)
        for yy, xx in ((yn, xn), (yn, x), (y, xn), (y, x))[: 4 if n < deep - 1 else 3]
    ]
    steps = 4
    width = depth // steps

    def columns(k):
        return pl.ds(k * width, width)

    q_load = pltpu.make_async_copy(q_ref, q_all.at[span(me)], load_sem.at[0])
    p_load = pltpu.make_async_copy(p_ref, p_own, load_sem.at[1])
    tables = [
        pltpu.make_async_copy(positives_ref, positives_own, load_sem.at[2]),
        pltpu.make_async_copy(mined_ref, mined_own, load_sem.at[3]),
        pltpu.make_async_copy(thresholds_ref, thresholds_own, load_sem.at[4]),
    ]
    q_load.start()
    p_load.start()
    for table in tables:
        table.start()

    has_up, has_down = z < deep - 1, z > 0
    above = device(y, jnp.minimum(z + 1, deep - 1), x)
    below = device(y, jnp.maximum(z - 1, 0), x)
    barrier = pltpu.get_barrier_semaphore()
    for to in (across, along, mate):
        pl.semaphore_signal(barrier, inc=1, device_id=to, device_id_type=MESH)

    @pl.when(has_up)
    def _():
        pl.semaphore_signal(barrier, inc=1, device_id=above, device_id_type=MESH)

    @pl.when(has_down)
    def _():
        pl.semaphore_signal(barrier, inc=1, device_id=below, device_id_type=MESH)

    pl.semaphore_wait(barrier, 3 + jnp.where(has_up, 1, 0) + jnp.where(has_down, 1, 0))
    q_load.wait()

    def pass_on(g, k, sem, to):
        ref = q_all.at[span(g), columns(k)]
        pltpu.make_async_remote_copy(
            src_ref=ref, dst_ref=ref, send_sem=sem, recv_sem=q_recv.at[g, k],
            device_id=to, device_id_type=MESH,
        ).start()

    whole = q_all.at[span(me)]

    @pl.when(core == 0)
    def _():
        pl.semaphore_wait(turn_sem, 1)

    for k in range(steps):
        @pl.when(has_up)
        def _():
            pass_on(me, k, own_send.at[0], above)

        @pl.when(has_down)
        def _():
            pass_on(me, k, own_send.at[1], below)

        pass_on(me, k, own_send.at[2], across)
        pass_on(me, k, own_send.at[3], along)
    waits.append((has_up, whole, own_send.at[0]))
    waits.append((has_down, whole, own_send.at[1]))
    waits.append((None, whole, own_send.at[2]))
    waits.append((None, whole, own_send.at[3]))
    p_load.wait()
    send(p_own, p_mate, mate_send.at[0], mate_recv.at[0], mate)
    for table in tables:
        table.wait()

    def mine(table):
        return jnp.concatenate(
            [table[(m * cores) * block : (m * cores + 1) * block] for m in range(deep * wide)], axis=0
        ), jnp.concatenate(
            [table[(m * cores + 1) * block : (m * cores + 2) * block] for m in range(deep * wide)], axis=0
        )

    mined_wide[...] = jnp.zeros_like(mined_wide)
    mined_wide[:negs, :] = mined_own[...].astype(jnp.float32)
    mined_wide[fields // 2 : fields // 2 + 1, :] = positives_own[...].astype(jnp.float32)
    mined_wide[fields // 2 + 1 : fields // 2 + 2, :] = thresholds_own[...]
    one_first, one_second = mine(jnp.transpose(mined_wide[...]))
    meta_ref[...] = jnp.transpose(jnp.where(core == 0, one_first, one_second))[:fields]
    meta_all[y] = meta_ref[...]
    send(meta_ref, meta_all.at[y], meta_send, meta_recv, device(yn, z, x))

    def column_step(h, up):
        source = z - h if up else z + h
        inside = source >= 0 if up else source < deep
        more = has_up if up else has_down
        far = above if up else below
        g = slot(y, jnp.clip(source, 0, deep - 1), x)
        sems = fwd_send.at[0 if up else 1, h - 1]

        def arrive(k):
            @pl.when(inside)
            def _():
                landed(q_all.at[span(g), columns(k)], q_recv.at[g, k])

                @pl.when(more)
                def _():
                    pass_on(g, k, sems.at[0], far)

                pass_on(g, k, sems.at[1], across)
                pass_on(g, k, sems.at[2], along)

        waits.append((inside & more, whole, sems.at[0]))
        waits.append((inside, whole, sems.at[1]))
        waits.append((inside, whole, sems.at[2]))
        return arrive

    def corner_step(source, inside, sem):
        at = jnp.clip(source, 0, deep - 1)
        gx, gy = slot(y, at, xn), slot(yn, at, x)

        def forward(k):
            g, to, n = (gx, along, 0) if k % 2 == 0 else (gy, across, 1)

            def go():
                landed(q_all.at[span(g), columns(k)], q_recv.at[g, k])
                pass_on(g, k, sem.at[n], to)

            if inside is None:
                go()
            else:
                pl.when(inside)(go)

        waits.append((inside, q_all.at[span(me), left], sem.at[0]))
        waits.append((inside, q_all.at[span(me), left], sem.at[1]))
        return forward

    def masks():
        landed(meta_all.at[yn], meta_recv)
        mt = jnp.concatenate([meta_all[a] for a in range(rows)], axis=1)
        at = lax.broadcasted_iota(jnp.int32, (2 * own, queries), 0)
        first = ((chip * cores + core) * rows + y) * own
        second = ((chip * cores + (1 - core)) * rows + y) * own
        ids = jnp.where(at < own, at + first, at - own + second).astype(jnp.float32)
        positive = ids == mt[fields // 2 : fields // 2 + 1, :]
        kept = positive
        for n in range(negs):
            kept = kept | (ids == mt[n : n + 1, :])
        positive_mask[...] = positive.astype(jnp.float32)
        kept_mask[...] = kept.astype(jnp.float32)
        margin[...] = mt[fields // 2 + 1 : fields // 2 + 2, :]

    corners = [corner_step(z, None, diag_send.at[0, 0])]
    for h in range(1, deep):
        arrivals = [column_step(h, True), column_step(h, False)]
        for k in range(steps):
            for go in arrivals:
                go(k)
            for go in corners:
                go(k)
        if h == 1:
            @pl.when(core == 1)
            def _():
                pl.semaphore_signal(turn_sem, inc=1, device_id=mate, device_id_type=MESH)

        if h == 1:
            masks()
        corners = [
            corner_step(z - h, z - h >= 0, diag_send.at[0, h]),
            corner_step(z + h, z + h < deep, diag_send.at[1, h]),
        ]
    for k in range(steps):
        for go in corners:
            go(k)
    landed(p_mate, mate_recv.at[0])

    for k in range(steps):
        for b in range(deep):
            zb = turn(z, b, deep)
            g = slot(yn, zb, x) if k % 2 == 0 else slot(y, zb, xn)
            gd = slot(yn, zb, xn)
            landed(q_all.at[span(g), columns(k)], q_recv.at[g, k])
            landed(q_all.at[span(gd), columns(k)], q_recv.at[gd, k])
        ks = columns(k)
        q_piece = q_all[:, ks]
        for at, p_part in ((0, p_own), (own, p_mate)):
            value = lax.dot_general(
                p_part[:, ks], q_piece, (((1,), (1,)), ((), ())), preferred_element_type=jnp.float32
            )
            if k:
                scores[at : at + own, :] += value
            else:
                scores[at : at + own, :] = value

    sc = scores[...] * inv_temp
    positive = positive_mask[...] > 0.0
    picked_here = jnp.sum(jnp.where(positive, sc, 0.0), axis=0, keepdims=True)
    kept = kept_mask[...] > 0.0
    held_here = jnp.max(jnp.where(kept, sc, -jnp.inf), axis=0, keepdims=True)
    pick_out[...] = jnp.concatenate([picked_here, held_here], axis=1)
    for n, peer in enumerate(peers):
        send(pick_out, pick_all.at[me], pick_send.at[n], pick_recv.at[me], device(*peer))
    pick_all[me] = pick_out[...]
    for peer in peers:
        g = slot(*peer)
        landed(pick_all.at[g], pick_recv.at[g])
    picks = pick_all[...]
    picked = jnp.sum(picks[:, :, :queries], axis=0)
    held = jnp.max(picks[:, :, queries:], axis=0)
    v = sharpness * (sc - picked - margin[...])
    penalty = jnp.maximum(v, 0.0) + jnp.log1p(jnp.exp(-jnp.abs(v)))
    grown = jnp.exp(jnp.where(kept, sc, sc - penalty) - held)
    sum_here = jnp.sum(grown, axis=0, keepdims=True)
    stat_out[...] = sum_here
    for n, peer in enumerate(peers):
        send(stat_out, stat_all.at[me], stat_send.at[n], stat_recv.at[me], device(*peer))
    stat_all[me] = sum_here
    grown_t[...] = jnp.transpose(grown)
    positive_t[...] = jnp.transpose(positive_mask[...])
    for peer in peers:
        g = slot(*peer)
        landed(stat_all.at[g], stat_recv.at[g])
    total = jnp.sum(stat_all[...], axis=0)
    factor = 1.0 / total
    factor_t = jnp.transpose(jnp.broadcast_to(factor, (8, queries)))[:, :1]
    grad_t = ((grown_t[...] * factor_t - positive_t[...]) * inv_temp).astype(jnp.bfloat16)

    cuts = 8
    cut = depth // cuts
    parts = 4
    share = depth // parts
    per = parts // 2
    mix = [k for pair in zip(range(per), range(per, parts)) for k in pair]
    def area(k, wrap=False):
        return pl.ds((k % per if wrap else k) * share, share)

    def post(src, dst, send_sem, recv_sem, to):
        pltpu.make_async_remote_copy(
            src_ref=src, dst_ref=dst, send_sem=send_sem, recv_sem=recv_sem,
            device_id=to, device_id_type=MESH,
        ).start()

    def route(k):
        return (along, across) if k < per else (across, along)

    def diagonal(n, k):
        gd = slot(yn, targets[n], xn)
        into = diag_in_y if k < per else diag_in_x
        post(
            part_low.at[span(gd), area(k)], into.at[n, :, area(k, True)],
            rd_send.at[n, k // per], rd_recv.at[n, k], route(k)[0],
        )

    def plain(n, k):
        g, into = (slot(yn, targets[n], x), in_y) if k < per else (slot(y, targets[n], xn), in_x)
        post(
            part_low.at[span(g), area(k)], into.at[n, :, area(k)],
            ru_send.at[n, k // per], ru_recv.at[n, k], route(k)[0],
        )

    def merged(n, k):
        g = slot(y, targets[n], xn) if k < per else slot(yn, targets[n], x)
        got, out, into = (diag_in_y, merge_x, in_x) if k < per else (diag_in_x, merge_y, in_y)
        landed(got.at[n, :, area(k, True)], rd_recv.at[n, k])
        out[n, :, area(k, True)] = (
            part[span(g), area(k)] + got[n, :, area(k, True)].astype(jnp.float32)
        ).astype(jnp.bfloat16)
        post(
            out.at[n, :, area(k, True)], into.at[n, :, area(k)],
            rm_send.at[n, k // per], rm_recv.at[n, k], route(k)[1],
        )

    def z_buffers(n):
        return (z_out_full, z_in_full) if n >= deep else (z_out, z_in)

    def settle(n, k):
        landed((in_y if k < per else in_x).at[n, :, area(k)], ru_recv.at[n, k])
        landed((in_x if k < per else in_y).at[n, :, area(k)], rm_recv.at[n, k])
        g = slot(y, targets[n], x)
        value = (
            part[span(g), area(k)]
            + in_x[n, :, area(k)].astype(jnp.float32)
            + in_y[n, :, area(k)].astype(jnp.float32)
        )
        if n < deep - 1:
            out, into = z_buffers(n)
            out[n, :, area(k)] = value.astype(out.dtype)
            post(
                out.at[n, :, area(k)], into.at[z, :, area(k)],
                z_send.at[n], z_recv.at[z, k], device(y, targets[n], x),
            )
        else:
            plane[:, area(k)] = value

    for k in mix:
        value = jnp.dot(grad_t[:, :own], p_own[:, area(k)], preferred_element_type=jnp.float32) + jnp.dot(
            grad_t[:, own:], p_mate[:, area(k)], preferred_element_type=jnp.float32
        )
        part[:, area(k)] = value
        part_low[:, area(k)] = value.astype(jnp.bfloat16)
        diagonal(0, k)
    for k in mix:
        diagonal(1, k)
    for k in mix:
        plain(0, k)

    losses = jnp.broadcast_to(held + jnp.log(total) - picked, (8, queries))
    loss_ref[...] = pltpu.roll(losses, lax.rem(queries - me * block, queries), 1)[:1, :block]
    grad = ((grown * factor - positive.astype(jnp.float32)) * inv_temp).astype(jnp.bfloat16)

    @pl.loop(0, cuts)
    def _(k):
        ks = pl.ds(pl.multiple_of(k * cut, lane), cut)
        gp_out[:, ks] = jnp.dot(grad[own:, :], q_all[:, ks], preferred_element_type=jnp.float32)

    send(gp_out, gp_in, mate_send.at[1], mate_recv.at[1], mate)

    for n in range(deep):
        for k in mix:
            merged(n, k)
            if n + 2 < deep:
                diagonal(n + 2, k)
        if n + 1 < deep:
            for k in mix:
                plain(n + 1, k)
        if n:
            for k in mix:
                settle(n - 1, k)

    landed(gp_in, mate_recv.at[1])

    @pl.loop(0, cuts)
    def _(k):
        ks = pl.ds(pl.multiple_of(k * cut, lane), cut)
        gp_ref[:, ks] = (
            jnp.dot(grad[:own, :], q_all[:, ks], preferred_element_type=jnp.float32) + gp_in[:, ks]
        )

    for k in mix:
        settle(deep - 1, k)
        value = plane[:, area(k)]
        for n in range(deep - 1):
            into = z_buffers(n)[1]
            landed(into.at[targets[n], :, area(k)], z_recv.at[targets[n], k])
            value = value + into[targets[n], :, area(k)].astype(jnp.float32)
        gq_ref[:, area(k)] = value
    for n in range(deep):
        for side in range(2):
            for sem in (rd_send, ru_send, rm_send):
                waits.append((None, merge_x.at[n], sem.at[n, side]))
        if n < deep - 1:
            waits.append((None, z_buffers(n)[0].at[n], z_send.at[n]))
    for inside, ref, sem in waits:
        if inside is None:
            landed(ref, sem)
        else:
            pl.when(inside)(functools.partial(landed, ref, sem))
    for copy in sent:
        copy.wait_send()


def store_kernel(loss_ref, gq_ref, gp_ref, loss_out, gq_out, gp_out, sems):
    copies = [
        pltpu.make_async_copy(source, out, sems.at[n])
        for n, (source, out) in enumerate(((gp_ref, gp_out), (gq_ref, gq_out), (loss_ref, loss_out)))
    ]
    for copy in copies:
        copy.start()
    for copy in copies:
        copy.wait()


def on_device(queries, passages, positives, hard_negatives, thresholds):
    rows, columns = lax.axis_size("row"), lax.axis_size("col")
    wide = rows
    deep = columns // (cores * wide)
    block, depth = queries.shape
    own = passages.shape[0]
    negs = hard_negatives.shape[1]
    run = deep * wide * block
    fits = rows == 2 and columns % (cores * wide) == 0 and deep > 1 and deep % 2 == 0
    fits = fits and block % 16 == 0 and run % lane == 0 and negs <= fields // 2 and depth % 1024 == 0
    if not fits:
        return general_plan(queries, passages, positives, hard_negatives, thresholds)
    groups = rows * deep * wide
    total = groups * block
    half = depth // 2
    low, full = jnp.bfloat16, jnp.float32
    dma = pltpu.SemaphoreType.DMA
    results = pl.pallas_call(
        functools.partial(step_kernel, rows, wide, deep, negs),
        out_shape=(
            jax.ShapeDtypeStruct((1, block), full),
            jax.ShapeDtypeStruct((block, depth), full),
            jax.ShapeDtypeStruct((own, depth), full),
        ),
        in_specs=[pl.BlockSpec(memory_space=pltpu.HBM)] * 5,
        out_specs=[pl.BlockSpec(memory_space=pltpu.VMEM)] * 3,
        scratch_shapes=[
            pltpu.VMEM((cores * own, total), full),
            pltpu.VMEM((cores * own, total), full),
            pltpu.VMEM((1, total), full),
            pltpu.VMEM((total, cores * own), full),
            pltpu.VMEM((total, cores * own), full),
            pltpu.VMEM((own, depth), low),
            pltpu.VMEM((1, positives.shape[0]), jnp.int32),
            pltpu.VMEM((negs, positives.shape[0]), jnp.int32),
            pltpu.VMEM((1, positives.shape[0]), full),
            pltpu.VMEM((total, depth), low),
            pltpu.VMEM((own, depth), low),
            pltpu.VMEM((lane, columns * block), full),
            pltpu.VMEM((fields, run), full),
            pltpu.VMEM((rows, fields, run), full),
            pltpu.VMEM((cores * own, total), full),
            pltpu.VMEM((1, 2 * total), full),
            pltpu.VMEM((groups, 1, 2 * total), full),
            pltpu.VMEM((1, total), full),
            pltpu.VMEM((groups, 1, total), full),
            pltpu.VMEM((total, depth), full),
            pltpu.VMEM((total, depth), low),
            pltpu.VMEM((own, depth), full),
            pltpu.VMEM((own, depth), full),
            pltpu.VMEM((deep, block, half), low),
            pltpu.VMEM((deep, block, half), low),
            pltpu.VMEM((deep, block, half), low),
            pltpu.VMEM((deep, block, half), low),
            pltpu.VMEM((deep, block, depth), low),
            pltpu.VMEM((deep, block, depth), low),
            pltpu.VMEM((block, depth), full),
            pltpu.VMEM((deep, block, depth), low),
            pltpu.VMEM((deep, block, depth), low),
            pltpu.VMEM((deep, block, depth), full),
            pltpu.VMEM((deep, block, depth), full),
            dma((5,)), dma((4,)), dma((2, deep, 3)), dma((2, deep, 2)), dma((groups, 4)),
            dma((2,)), dma((2,)), dma, dma,
            dma((groups,)), dma((groups,)), dma((groups,)), dma((groups,)),
            dma((deep, 2)), dma((deep, 4)), dma((deep, 2)), dma((deep, 4)),
            dma((deep, 2)), dma((deep, 4)), dma((deep,)), dma((deep, 4)),
            pltpu.SemaphoreType.REGULAR,
        ],
        compiler_params=pltpu.CompilerParams(
            collective_id=0, has_side_effects=True, vmem_limit_bytes=46 * 1024 * 1024
        ),
    )(*(
        pltpu.with_memory_space_constraint(a, pltpu.HBM)
        for a in (queries, passages, positives[None], hard_negatives.T, thresholds[None])
    ))
    losses, grad_queries, grad_passages = pl.pallas_call(
        store_kernel,
        out_shape=[jax.ShapeDtypeStruct(a.shape, a.dtype) for a in results],
        in_specs=[pl.BlockSpec(memory_space=pltpu.VMEM)] * 3,
        out_specs=[pl.BlockSpec(memory_space=pltpu.HBM)] * 3,
        scratch_shapes=[dma((3,))],
        compiler_params=pltpu.CompilerParams(vmem_limit_bytes=8 * 1024 * 1024),
    )(*results)
    return (losses[0], grad_queries, grad_passages)


def solution(mesh):
    placed = (P(("row", "col"), None), P(("col", "row"), None), P("row"), P("row", None), P("row"))
    return jax.shard_map(
        on_device,
        mesh=mesh,
        in_specs=placed,
        out_specs=(P(("row", "col")), P(("row", "col"), None), P(("col", "row"), None)),
        check_vma=False,
    )
```
